32 devices in a mesh: groups: 2 (over y), word: 4 (over z), sub: 4 (over x, core).
Axes of the slice: x: 2, y: 2, z: 4, core: 2. Of those that a mesh axis runs over, the one named last changes fastest.
Arguments:
- word_ids: int32 [4, 32, 512], P('word', None, 'groups'), parts along dimension 2, may hold values from 0 to 32767
- word_weights: float32 [4, 32, 512], P('word', None, 'groups'), parts along dimension 2, may hold values from 0.25 to 12
- neighbours: int32 [50, 512], P(None, 'groups'), parts along dimension 1, may hold values from 0 to 255
- descriptors: bfloat16 [512, 128, 128], P(('groups', 'word'), 'sub'), parts along dimension 0, may hold values from -6 to 6
- keypoint_count: int32 [512], P('groups'), parts along dimension 0, may hold values from 32 to 128
- send_table: int32 [8, 4, 4, 2], P('groups'), parts along dimension 0, may hold values from 0 to 63
- pair_slots: int32 [8, 4, 32, 2], P(('groups', 'word'), 'sub'), parts along dimension 0, may hold values from 0 to 7, as said below
Outputs:
- similarity: float32 [512, 50], P(('groups', 'word', 'sub')), parts along dimension 0
- nearest: float32 [8, 4, 32, 128], P(('groups', 'word'), 'sub'), parts along dimension 0
- margin: float32 [8, 4, 32, 128], P(('groups', 'word'), 'sub'), parts along dimension 0
The draws below stay inside these ranges and needn't reach their ends.
There are 2 independent parts, one for each index of `groups`. The reference program is written for one: setup_inputs(seed, part) draws one part's arguments, and reference() takes and returns one part's arrays. A program takes and returns all parts, laid end to end along the dimension named above; each array names one. Nothing has to cross between parts.
Inputs may be any that keep to these rules, and one draw needn't show every extreme that they name: `word_ids`: each image has 32 word occurrences in every vocabulary shard, given as word numbers within that shard; a number may repeat. `keypoint_count`: keypoint slots at and beyond an image's count are padding. send_table[v, w, s, c] is an image counted among word index v's 64 stored images; every device receives exactly 2 images from every word index, and one image may go to many devices. `pair_slots`: the two slots of a pair are different slots among the 8 of that device, the query first.
All inputs are finite; a program needn't handle non-finite values.
Results may differ from the reference program's by a relative error of at most 0.0003.
Values may be sent and summed in bfloat16 or wider, within the bound.
A program may use at most 64 MiB of HBM per device.

```python
import math
import jax
import jax.numpy as jnp
import numpy as np
from jax import lax

DESC = 128
VOCAB_DEV = 32768
TOPK = 50
CAP = 2
KP = 128
IMG_DEV = 64
SLOTS = 32
PAIR_DEV = 32
SHARDS = 4
SUBS = 4
IMAGES = 256
HELD = 8


def draw_word_weights(key, part):
    array_shape = (SHARDS, SLOTS, IMAGES)
    shard_ramp = 1.0 + 2.0 * jnp.arange(SHARDS, dtype=jnp.float32) / max(SHARDS - 1, 1)
    factor = jnp.exp(jax.random.uniform(key, array_shape, jnp.float32, math.log(0.25), math.log(4.0)))
    return (factor * shard_ramp[:, None, None]).astype(jnp.float32)


def draw_pair_slots(key, part):
    first_key, second_key = jax.random.split(key)
    query_slot = jax.random.randint(first_key, (SHARDS, SUBS, PAIR_DEV, 1), 0, HELD)
    offset = jax.random.randint(second_key, (SHARDS, SUBS, PAIR_DEV, 1), 1, HELD)
    return jnp.concatenate([query_slot, (query_slot + offset) % HELD], axis=3).astype(jnp.int32)


def plant(array, key, low, high):
    longest = array.shape.index(max(array.shape))
    spots = []
    for shift in (0, 1):
        where = [jax.random.randint(jax.random.fold_in(key, axis), (), 0, length) for axis, length in enumerate(array.shape)]
        where[longest] = (where[longest] + shift) % array.shape[longest]
        spots.append(tuple(where))
    return array.at[spots[0]].set(low).at[spots[1]].set(high)


def block_scale(rng, shape, shards, low, largest):
    gain, own = 1.0, jax.random.fold_in(rng, 6)
    for dim, blocks in shards:
        heights = jnp.exp(jax.random.uniform(jax.random.fold_in(own, dim), (blocks,), jnp.float32, low / len(shards), largest / len(shards)))
        gain = gain * jnp.repeat(heights, shape[dim] // blocks).reshape([-1 if axis == dim else 1 for axis in range(len(shape))])
    return gain


def rank_table(count, lean):
    weights = [(1 << 20) // math.isqrt(rank ** lean) + 1 for rank in range(1, count + 1)]
    spread = 1 + sum(weights) // (1 << 30)
    return np.cumsum(np.array([max(1, weight // spread) for weight in weights]))


def skewed_ids(stream_key, dims, amount, lean):
    grid = rank_table(amount, lean)
    ticket = jax.random.randint(jax.random.fold_in(stream_key, 1), dims, 0, int(grid[amount - 1]))
    standing = jnp.searchsorted(jnp.asarray(grid, jnp.int32), ticket, side="right")
    return jax.random.permutation(jax.random.fold_in(stream_key, 2), amount)[standing].astype(jnp.int32)


def noise(stream_key, extent, scale, most, cuts=(), kind=jnp.bfloat16):
    drawn = jax.random.normal(stream_key, extent, jnp.float32) * scale
    if len(cuts) > 0:
        drawn = block_scale(stream_key, extent, cuts, -0.22, 0.18) * drawn
    return jnp.clip(drawn, min=-most, max=most).astype(kind)


def setup_inputs(seed: int = 0, part: int = 0) -> dict:
    key_of = jax.random.split(jax.random.key(seed), 8)
    own_keys = jax.random.split(jax.random.fold_in(key_of[7], part), 8)
    word_ids = plant(skewed_ids(own_keys[0], (SHARDS, SLOTS, IMAGES), VOCAB_DEV, 2), jax.random.fold_in(own_keys[0], 3), 0, VOCAB_DEV - 1).astype(jnp.int32)
    word_weights = draw_word_weights(jax.random.fold_in(jax.random.fold_in(key_of[7], part), 71), part)
    neighbours = plant(jax.random.randint(own_keys[2], (TOPK, IMAGES), 0, IMAGES), jax.random.fold_in(own_keys[2], 1), 0, IMAGES - 1).astype(jnp.int32)
    descriptors = noise(own_keys[3], (IMAGES, DESC, KP), 1.0, 6.0, ((0, 4), (1, 4)))
    keypoint_count = plant(jax.random.randint(own_keys[4], (IMAGES,), KP // 4, KP + 1), jax.random.fold_in(own_keys[4], 1), KP // 4, KP).astype(jnp.int32)
    send_table = plant(jax.random.randint(own_keys[5], (SHARDS, SHARDS, SUBS, CAP), 0, IMG_DEV), jax.random.fold_in(own_keys[5], 1), 0, IMG_DEV - 1).astype(jnp.int32)
    pair_slots = draw_pair_slots(jax.random.fold_in(jax.random.fold_in(key_of[7], part), 71), part)
    return dict(word_ids=word_ids, word_weights=word_weights, neighbours=neighbours, descriptors=descriptors, keypoint_count=keypoint_count, send_table=send_table, pair_slots=pair_slots)


def pair_products(row_ids, row_values, other_ids, other_values):
    matches = row_ids[:, :, :, None] == other_ids[:, :, None, :]
    weights = row_values[:, :, :, None] * other_values[:, :, None, :]
    return lax.optimization_barrier(jnp.sum(jnp.where(matches, weights, jnp.float32(0.0)), axis=(2, 3)))

def blocked(function, arrays, block_width):
    row_total = arrays[0].shape[0]
    block_rows = math.gcd(row_total, block_width)
    shaped = tuple((member.reshape((row_total // block_rows, block_rows) + member.shape[1:]) for member in arrays))
    result = lax.map(lambda bundle: function(*bundle), shaped)
    return jax.tree.map(lambda output: output.reshape((row_total,) + output.shape[2:]), result)

def finish(squared, query_count, refer_count, feature_width):
    positions = jnp.arange(squared.shape[-1], dtype=jnp.int32)
    masked = jnp.where(positions[None, None, :] < refer_count[:, None, None], squared, jnp.inf)
    best_value = lax.optimization_barrier(jnp.min(masked, axis=-1))
    at_best = masked == best_value[..., None]
    ties = lax.optimization_barrier(jnp.sum(at_best.astype(jnp.int32), axis=-1))
    others = lax.optimization_barrier(jnp.min(jnp.where(at_best, jnp.inf, masked), axis=-1))
    second = jnp.where(ties > 1, best_value, others)
    live_rows = positions[None, :] < query_count[:, None]
    nearest = jnp.where(live_rows, best_value / feature_width, jnp.float32(0.0))
    margin = jnp.where(live_rows, (second - best_value) / feature_width, jnp.float32(0.0))
    return (nearest, margin)

def shard_terms(shard_ids, shard_values, neighbours):

    def self_block(row_ids, row_values):
        return pair_products(row_ids[:, None, :], row_values[:, None, :], row_ids[:, None, :], row_values[:, None, :])[:, 0]

    def neighbour_block(row_ids, row_values, row_neighbours):
        return pair_products(row_ids[:, None, :], row_values[:, None, :], shard_ids[row_neighbours], shard_values[row_neighbours])
    self_terms = blocked(self_block, (shard_ids, shard_values), 256)
    cross_terms = blocked(neighbour_block, (shard_ids, shard_values, neighbours), 16)
    return (self_terms, cross_terms)

def reference(word_ids, word_weights, neighbours, descriptors, keypoint_count, send_table, pair_slots):
    word_rows = jnp.transpose(word_ids, (0, 2, 1))
    weight_rows = jnp.transpose(word_weights, (0, 2, 1))
    neighbour_rows = jnp.transpose(neighbours, (1, 0))
    self_terms, cross_terms = lax.map(lambda bundle: shard_terms(bundle[0], bundle[1], neighbour_rows), (word_rows, weight_rows))
    norm_sq = lax.optimization_barrier(jnp.sum(self_terms, axis=0))
    dot_sums = lax.optimization_barrier(jnp.sum(cross_terms, axis=0))
    similarity = dot_sums / jnp.sqrt(norm_sq[:, None] * norm_sq[neighbour_rows])
    source_base = (jnp.arange(SHARDS, dtype=jnp.int32) * IMG_DEV)[:, None, None, None]
    slot_image = jnp.transpose(send_table + source_base, (1, 2, 0, 3)).reshape(SHARDS, SUBS, HELD)
    query_image = jnp.take_along_axis(slot_image, pair_slots[:, :, :, 0], axis=2).reshape(-1)
    refer_image = jnp.take_along_axis(slot_image, pair_slots[:, :, :, 1], axis=2).reshape(-1)
    squared_norm = blocked(lambda member: lax.optimization_barrier(jnp.sum(jnp.square(member.astype(jnp.float32)), axis=1)), (descriptors,), 64)

    def match_block(query_rows, refer_rows):
        query_desc = descriptors[query_rows].astype(jnp.float32)
        refer_desc = descriptors[refer_rows].astype(jnp.float32)
        inner_prod = jnp.einsum('bfm,bfn->bmn', query_desc, refer_desc, precision=lax.Precision.HIGHEST)
        squared = squared_norm[query_rows][:, :, None] + squared_norm[refer_rows][:, None, :] - 2.0 * inner_prod
        return finish(squared, keypoint_count[query_rows], keypoint_count[refer_rows], DESC)
    nearest, margin = blocked(match_block, (query_image, refer_image), 4)
    nearest = nearest.reshape(SHARDS, SUBS, PAIR_DEV, KP)
    margin = margin.reshape(SHARDS, SUBS, PAIR_DEV, KP)
    return (similarity, nearest, margin)
```

```python
import functools

import jax
import jax.numpy as jnp
from jax import lax
from jax.experimental import pallas as pl
from jax.experimental.pallas import tpu as pltpu
from jax.sharding import PartitionSpec as P

MESH = pl.DeviceIdType.MESH
LANES = 128
LIMIT = 40 * 1024 * 1024
F32, BF16, I32 = jnp.float32, jnp.bfloat16, jnp.int32


def ceil_to(value, step):
    return (value + step - 1) // step * step


def loop(count, limit, body):
    if count <= limit:
        for i in range(count):
            body(i)
    else:
        lax.fori_loop(0, count, lambda i, carry: (body(i), carry)[1], 0)


def pieces(x):
    first = x.astype(BF16)
    rest = x - first.astype(F32)
    second = rest.astype(BF16)
    third = (rest - second.astype(F32)).astype(BF16)
    return first, second, third


def dot(a, b):
    return lax.dot_general(a, b, (((1,), (0,)), ((), ())), preferred_element_type=F32)


def onehot(want, rows):
    numbers = lax.broadcasted_iota(I32, (rows, want.shape[-1]), 0)
    return jnp.where(numbers == want, F32(1.0), F32(0.0)).astype(BF16)


def kernel(
    W, S, dims,
    ids_hbm, wts_hbm, nb_hbm, desc_hbm, cnt_hbm, tab_hbm, slot_hbm,
    sim_ref, near_ref, marg_ref,
    ids_ref, wts_ref, nb_ref, desc_ref, cnt_ref, to_ref, from_ref, slot_ref,
    outd, held, table, nbf, own, hot, got, part_out, part_in,
    qs, rt, sqb, info, low_s, next_s, info_s,
    dsend, drecv, psend, precv, inputs, go,
):
    B, I, K, R, KK, J, C, TR, KP, NP, H = dims
    me_g, me_w, me_s = lax.axis_index("groups"), lax.axis_index("word"), lax.axis_index("sub")
    n = W * S
    stored, feats, width = desc_ref.shape

    def turn(step):
        if W & (W - 1):
            return (me_w + step) % W
        word, bit = me_w, 1
        while bit < W:
            word += step // bit % 2 * (1 - me_w // bit % 2 * 2) * bit
            bit *= 2
        return word

    def word_at(k):
        return k + jnp.where(me_w <= k, 1, 0)

    def near(j):
        return (me_s + 1 + j) % S

    def load(sem, source, target):
        return pltpu.make_async_copy(source, target, inputs.at[sem])

    first = [
        load(0, tab_hbm.at[me_w], to_ref),
        load(1, desc_hbm, desc_ref),
    ]
    rest = [
        load(2, ids_hbm, ids_ref),
        load(3, wts_hbm, wts_ref),
        load(4, nb_hbm, nb_ref),
        load(5, tab_hbm.at[:, me_w], from_ref),
        load(6, cnt_hbm, cnt_ref),
        load(7, slot_hbm, slot_ref),
    ]
    for copy in first:
        copy.start()

    def words(above, body):
        for_each = lambda k: pl.when((k >= me_w) if above else (k < me_w))(lambda: body(word_at(k)))
        loop(W - 1, 4, for_each)

    def subs(above, body):
        loop(S, 8, lambda s: pl.when((s > me_s) if above else (s < me_s))(lambda: body(s)))

    barrier = pltpu.get_barrier_semaphore()

    def signal(sem, w, s):
        pl.semaphore_signal(sem, inc=1, device_id=(me_g, w, s), device_id_type=MESH)

    subs(True, lambda s: signal(barrier, me_w, s))
    words(True, lambda w: loop(S, 8, lambda s: signal(barrier, w, s)))
    for copy in rest:
        copy.start()
    lower = me_w * S + me_s
    pl.when(lower > 0)(lambda: pl.semaphore_wait(barrier, lower))
    words(False, lambda w: loop(S, 8, lambda s: signal(go.at[me_w], w, s)))
    subs(False, lambda s: signal(go.at[me_w], me_w, s))
    for copy in first:
        copy.wait()

    def pick(slot, w, s):
        for c in range(C):
            outd[slot, c] = desc_ref[to_ref[w, c, s]]

    loop(W - 1, 4, lambda k: loop(S, 8, lambda s: pick(k * S + s, word_at(k), s)))
    loop(S, 8, lambda s: pick((W - 1) * S + s, me_w, s))
    for c in range(C):
        held[me_w, me_s, c] = desc_ref[to_ref[me_w, c, me_s]]

    def send(slot, w, s):
        pltpu.make_async_remote_copy(
            src_ref=outd.at[slot], dst_ref=held.at[me_w, me_s],
            send_sem=dsend, recv_sem=drecv.at[me_w],
            device_id=(me_g, w, s), device_id_type=MESH,
        ).start()

    def send_word(k):
        loop(S, 8, lambda s: send(k * S + s, word_at(k), s))

    def send_near(s):
        send((W - 1) * S + s, me_w, s)

    pl.when(me_w > 0)(lambda: send_word(0))
    subs(False, send_near)

    for copy in rest:
        copy.wait()

    ids = ids_ref[...]
    table[0:B] = (ids >> 8).astype(F32).astype(BF16)
    table[B : 2 * B] = (ids & 255).astype(F32).astype(BF16)
    for i, piece in enumerate(pieces(wts_ref[...])):
        table[(2 + i) * B : (3 + i) * B] = piece
    nbf[...] = jnp.zeros_like(nbf)
    nbf[0:K] = nb_ref[...]
    near_ids = nbf[...]
    table[TR : TR + KP] = (near_ids >> 8).astype(F32).astype(BF16)
    table[TR + KP : TR + 2 * KP] = (near_ids & 255).astype(F32).astype(BF16)

    chunk = min(I, 256)

    def self_norm(i):
        at = pl.ds(i * chunk if isinstance(i, int) else pl.multiple_of(i * chunk, chunk), chunk)
        here = ids_ref[:, at]
        total = jnp.zeros((B, chunk), F32)
        for a in range(B):
            total += jnp.where(here == ids_ref[a : a + 1, at], wts_ref[a : a + 1, at], F32(0.0))
        norm = jnp.sum(total * wts_ref[:, at], axis=0, keepdims=True)
        row = lax.broadcasted_iota(I32, (16, chunk), 0)
        block = jnp.zeros((16, chunk), F32)
        for k, piece in enumerate(pieces(norm)):
            block = jnp.where(row == k, piece.astype(F32), block)
        table[5 * B : TR, at] = block.astype(BF16)

    loop(I // chunk, 1, self_norm)

    def part_copy(d):
        w = word_at(d)
        return pltpu.make_async_remote_copy(
            src_ref=part_out.at[d], dst_ref=part_in.at[me_w - jnp.where(me_w > w, 1, 0)],
            send_sem=psend, recv_sem=precv,
            device_id=(me_g, w, me_s), device_id_type=MESH,
        )

    early = 2 * me_w < W - 1

    def due(d):
        low = jnp.logical_and(d >= 0, d < me_w)
        high = jnp.logical_and(d >= me_w, d < W - 1)
        return jnp.logical_or(low, jnp.logical_and(high, jnp.logical_not(early)))

    lane = lax.broadcasted_iota(I32, (1, LANES), 1)
    digit = lax.broadcasted_iota(I32, (KK, LANES), 0) == lax.broadcasted_iota(I32, (KK, LANES), 1) // R

    def target(d):
        w = jnp.where(d == W - 1, me_w, word_at(d))
        mine = dot(table[...], onehot((w * S + me_s) * R + lane % R, I))
        own[0:B] = mine[0:B] * 256.0 + mine[B : 2 * B]
        own[B : 2 * B] = mine[2 * B : 3 * B] + mine[3 * B : 4 * B] + mine[4 * B : 5 * B]
        listed = mine[TR : TR + KP] * 256.0 + mine[TR + KP : TR + 2 * KP]
        for j in range(J):
            chosen = jnp.where(digit, listed[j * KK : (j + 1) * KK], F32(0.0))
            want = jnp.sum(chosen, axis=0, keepdims=True).astype(I32)
            hot[:, j * LANES : (j + 1) * LANES] = onehot(want, I)
        pl.when(due(d - 1))(lambda: part_copy(d - 1).start())
        pl.when(jnp.logical_and(d >= 1, d < me_w))(lambda: send_word(d))
        got[...] = dot(table[0:TR], hot[...])
        cols = [slice(j * LANES, (j + 1) * LANES) for j in range(J)]
        words_of = [got[0:B, c] * 256.0 + got[B : 2 * B, c] for c in cols]
        total = [jnp.zeros((B, LANES), F32) for c in cols]
        for a in range(B):
            word, weight = own[a : a + 1], own[B + a : B + a + 1]
            for j in range(J):
                total[j] += jnp.where(words_of[j] == word, weight, F32(0.0))
        for j, c in enumerate(cols):
            values = got[2 * B : 3 * B, c] + got[3 * B : 4 * B, c] + got[4 * B : 5 * B, c]
            part_out[d, j : j + 1] = jnp.sum(total[j] * values, axis=0, keepdims=True)
            norms = got[5 * B : 5 * B + 1, c] + got[5 * B + 1 : 5 * B + 2, c] + got[5 * B + 2 : 5 * B + 3, c]
            part_out[d, J + j : J + j + 1] = norms
        part_out[d, 2 * J : 2 * J + 1] = (
            mine[5 * B : 5 * B + 1] + mine[5 * B + 1 : 5 * B + 2] + mine[5 * B + 2 : 5 * B + 3]
        )
    def targets(first, last):
        lax.fori_loop(first, last, lambda d, carry: (target(d), carry)[1], 0)

    def quota(e):
        return jnp.minimum(jnp.maximum(W - 2 - me_w + e, 1), W)

    def stage(e):
        targets(0 if isinstance(e, int) and e == 0 else jnp.where(e == 0, 0, quota(e - 1)), quota(e))
        if not isinstance(e, int):
            pl.when(e == 0)(near_stage)
            pl.when(e > 0)(lambda: far_stage(e))
        elif e == 0:
            near_stage()
        else:
            far_stage(e)

    def near_stage():
        pl.when(me_s < S - 1)(lambda: pl.semaphore_wait(go.at[me_w], S - 1 - me_s))
        subs(True, send_near)

    def far_stage(e):
        w = me_w + e
        pl.semaphore_wait(go.at[w], S)
        pl.when(early)(lambda: part_copy(w - 1).start())
        send_word(w - 1)

    loop(W, 4, lambda e: pl.when(me_w + e < W)(lambda: stage(e)))
    targets(quota(W - 1 - me_w), W)

    def arrive(i):
        w = turn(i)

        def arrived(slices):
            pltpu.make_async_remote_copy(
                src_ref=held.at[w, pl.ds(0, slices)], dst_ref=held.at[w, pl.ds(0, slices)],
                send_sem=dsend, recv_sem=drecv.at[w],
                device_id=(me_g, me_w, me_s), device_id_type=MESH,
            ).wait_recv()

        if isinstance(i, int):
            arrived(S if i > 0 else S - 1)
        else:
            pl.when(i > 0)(lambda: arrived(S))
            pl.when(i == 0)(lambda: arrived(S - 1))
        for c in range(C):
            h = w * C + c
            full = jnp.concatenate([held[w, s, c] for s in range(S)], axis=0)
            qs[h] = full
            wide = full.astype(F32)
            turned = jnp.transpose(wide)
            rt[h] = (turned * -2.0).astype(BF16)
            count = cnt_ref[w * stored + from_ref[w, c, me_s]]
            down = lax.broadcasted_iota(I32, (width, width), 0)
            square = jnp.sum(turned * turned, axis=1, keepdims=True)
            sqb[h] = jnp.where(down < count, square, F32(1e30))
            flat = jnp.sum(wide * wide, axis=0, keepdims=True)
            live = jnp.where(lax.broadcasted_iota(I32, (8, width), 1) < count, F32(1.0), F32(0.0))
            info[h] = jnp.where(lax.broadcasted_iota(I32, (8, width), 0) == 0, flat, live)

    loop(W - 1, 4, arrive)

    def whole(ref, send_sem, recv_sem):
        return pltpu.make_async_remote_copy(
            src_ref=ref, dst_ref=ref, send_sem=send_sem, recv_sem=recv_sem,
            device_id=(me_g, me_w, me_s), device_id_type=MESH,
        )

    whole(part_in.at[pl.ds(0, W - 1)], psend, precv).wait_recv()
    total = part_out[W - 1]
    for d in range(W - 1):
        total += part_in[d]
    cosine = total[0:J] / jnp.sqrt(total[2 * J : 2 * J + 1] * total[J : 2 * J])
    spread = lax.broadcasted_iota(I32, (R, LANES), 1) % R == lax.broadcasted_iota(I32, (R, LANES), 0)
    out_cols = ceil_to(K, LANES)
    deep = lax.broadcasted_iota(I32, (LANES, out_cols), 0) // R
    across = lax.broadcasted_iota(I32, (LANES, out_cols), 1)
    result = jnp.zeros((R, out_cols), F32)
    for j in range(J):
        place = jnp.where(across == deep + j * KK, F32(1.0), F32(0.0)).astype(BF16)
        for piece in pieces(jnp.where(spread, cosine[j : j + 1], F32(0.0))):
            result += dot(piece, place)
    sim_ref[...] = result[:, 0:K]

    arrive(W - 1)

    pairs = near_ref.shape[0]
    group = 8

    def match(i):
        for k in range(group):
            p = i * group + k
            q, r = slot_ref[0, p], slot_ref[1, p]
            inner = dot(rt[r], qs[q])
            base = sqb[r]
            tops = []
            for t in range(2):
                low = second = None
                for v in range(t, width // 8, 2):
                    x = base[v * 8 : v * 8 + 8] + inner[v * 8 : v * 8 + 8]
                    if low is None:
                        low = x
                    elif second is None:
                        low, second = jnp.minimum(low, x), jnp.maximum(low, x)
                    else:
                        second = jnp.minimum(second, jnp.maximum(low, x))
                        low = jnp.minimum(low, x)
                tops.append((low, second))
            (l0, s0), (l1, s1) = tops
            at = pl.ds(p * 8, 8)
            low_s[at] = jnp.minimum(l0, l1)
            next_s[at] = jnp.minimum(jnp.maximum(l0, l1), jnp.minimum(s0, s1))
            info_s[at] = info[q]

    loop(pairs // group, 4, match)

    rows = [pl.ds(i, pairs, stride=8) for i in range(8)]
    low, second = low_s[rows[0]], next_s[rows[0]]
    for at in rows[1:]:
        l1, s1 = low_s[at], next_s[at]
        second = jnp.minimum(jnp.maximum(low, l1), jnp.minimum(second, s1))
        low = jnp.minimum(low, l1)
    live = info_s[rows[1]] > 0.0
    features = F32(feats * S)
    near_ref[...] = jnp.where(live, (low + info_s[rows[0]]) / features, F32(0.0))
    marg_ref[...] = jnp.where(live, (second - low) / features, F32(0.0))

    whole(outd.at[pl.ds(0, n - 1)], dsend, drecv.at[0]).wait_send()
    whole(part_out.at[pl.ds(0, W - 1)], psend, precv).wait_send()


def finish(*refs):
    sems = refs[6]
    copies = [pltpu.make_async_copy(refs[i], refs[3 + i], sems.at[i]) for i in range(3)]
    for copy in copies:
        copy.start()
    for copy in copies:
        copy.wait()


def local(W, S, word_ids, word_weights, neighbours, descriptors, keypoint_count, send_table, pair_slots):
    B, I = word_ids.shape[1:]
    K = neighbours.shape[0]
    R = I // (W * S)
    KK = LANES // R
    J = -(-K // KK)
    C = send_table.shape[-1]
    TR = ceil_to(5 * B + 3, 16)
    KP = ceil_to(J * KK, 16)
    NP = ceil_to(2 * J + 1, 8)
    H = W * C
    stored, feats, width = descriptors.shape
    pairs = pair_slots.shape[2]
    vmem = pl.BlockSpec(memory_space=pltpu.VMEM)
    results = ((R, K), (pairs, width), (pairs, width))
    parts = pl.pallas_call(
        functools.partial(kernel, W, S, (B, I, K, R, KK, J, C, TR, KP, NP, H)),
        out_shape=tuple(pltpu.VMEM(shape, F32) for shape in results),
        in_specs=[pl.BlockSpec(memory_space=pltpu.HBM)] * 7,
        out_specs=(vmem, vmem, vmem),
        scratch_shapes=[
            pltpu.VMEM((B, I), I32),
            pltpu.VMEM((B, I), F32),
            pltpu.VMEM((K, I), I32),
            pltpu.VMEM(descriptors.shape, BF16),
            pltpu.SMEM(keypoint_count.shape, I32),
            pltpu.SMEM((W, C, S), I32),
            pltpu.SMEM((W, C, S), I32),
            pltpu.SMEM((2, pairs), I32),
            pltpu.VMEM((W * S, C, feats, width), BF16),
            pltpu.VMEM((W, S, C, feats, width), BF16),
            pltpu.VMEM((TR + 2 * KP, I), BF16),
            pltpu.VMEM((KP, I), I32),
            pltpu.VMEM((2 * B, LANES), F32),
            pltpu.VMEM((I, J * LANES), BF16),
            pltpu.VMEM((TR, J * LANES), F32),
            pltpu.VMEM((W, NP, LANES), F32),
            pltpu.VMEM((W, NP, LANES), F32),
            pltpu.VMEM((H, width, width), BF16),
            pltpu.VMEM((H, width, width), BF16),
            pltpu.VMEM((H, width, width), F32),
            pltpu.VMEM((H, 8, width), F32),
            pltpu.VMEM((pairs * 8, width), F32),
            pltpu.VMEM((pairs * 8, width), F32),
            pltpu.VMEM((pairs * 8, width), F32),
            pltpu.SemaphoreType.DMA,
            pltpu.SemaphoreType.DMA((W,)),
            pltpu.SemaphoreType.DMA,
            pltpu.SemaphoreType.DMA,
            pltpu.SemaphoreType.DMA((8,)),
            pltpu.SemaphoreType.REGULAR((W,)),
        ],
        compiler_params=pltpu.CompilerParams(
            collective_id=0, has_side_effects=True, vmem_limit_bytes=LIMIT
        ),
    )(*(pltpu.with_memory_space_constraint(operand, pltpu.HBM) for operand in (
        word_ids[0], word_weights[0], neighbours, descriptors,
        keypoint_count, jnp.swapaxes(send_table, 2, 3), jnp.swapaxes(pair_slots, 2, 3)[0, 0],
    )))
    similarity, nearest, margin = pl.pallas_call(
        finish,
        out_shape=tuple(jax.ShapeDtypeStruct(shape, F32) for shape in results),
        in_specs=[pl.BlockSpec(memory_space=pl.ANY)] * 3,
        out_specs=(pl.BlockSpec(memory_space=pltpu.HBM),) * 3,
        scratch_shapes=[pltpu.SemaphoreType.DMA((3,))],
        compiler_params=pltpu.CompilerParams(vmem_limit_bytes=LIMIT),
    )(*parts)
    return similarity, nearest[None, None], margin[None, None]


def solution(mesh):
    in_specs = (
        P("word", None, "groups"),
        P("word", None, "groups"),
        P(None, "groups"),
        P(("groups", "word"), "sub", None),
        P("groups"),
        P("groups", None, None, None),
        P(("groups", "word"), "sub", None, None),
    )
    out_specs = (
        P(("groups", "word", "sub"), None),
        P(("groups", "word"), "sub", None, None),
        P(("groups", "word"), "sub", None, None),
    )
    body = functools.partial(local, mesh.shape["word"], mesh.shape["sub"])
    return jax.shard_map(body, mesh=mesh, in_specs=in_specs, out_specs=out_specs, check_vma=False)
```

```python
import functools

import jax
import jax.numpy as jnp
from jax import lax
from jax.experimental import pallas as pl
from jax.experimental.pallas import tpu as pltpu
from jax.sharding import PartitionSpec as P

MESH = pl.DeviceIdType.MESH
LANES = 128
LIMIT = 40 * 1024 * 1024
F32, BF16, I32 = jnp.float32, jnp.bfloat16, jnp.int32


def ceil_to(value, step):
    return (value + step - 1) // step * step


def loop(count, limit, body):
    if count <= limit:
        for i in range(count):
            body(i)
    else:
        lax.fori_loop(0, count, lambda i, carry: (body(i), carry)[1], 0)


def pieces(x):
    first = x.astype(BF16)
    rest = x - first.astype(F32)
    second = rest.astype(BF16)
    third = (rest - second.astype(F32)).astype(BF16)
    return first, second, third


def dot(a, b):
    return lax.dot_general(a, b, (((1,), (0,)), ((), ())), preferred_element_type=F32)


def onehot(want, rows):
    numbers = lax.broadcasted_iota(I32, (rows, want.shape[-1]), 0)
    return jnp.where(numbers == want, F32(1.0), F32(0.0)).astype(BF16)


def kernel(
    W, S, dims,
    ids_hbm, wts_hbm, nb_hbm, desc_hbm, cnt_hbm, tab_hbm, slot_hbm,
    sim_ref, near_ref, marg_ref,
    ids_ref, wts_ref, nb_ref, desc_ref, cnt_ref, to_ref, from_ref, slot_ref,
    outd, held, table, nbf, own, wanted, got_0, got_1, part_out, part_in,
    qs, rt, sqb, info, low_s, next_s, info_s,
    dsend, drecv, psend, precv, inputs, go,
):
    B, I, K, R, KK, J, C, TR, KP, NP, H = dims
    gots = got_0, got_1
    me_g, me_w, me_s = lax.axis_index("groups"), lax.axis_index("word"), lax.axis_index("sub")
    n = W * S
    stored, feats, width = desc_ref.shape

    def turn(step):
        if isinstance(step, int) and step == 0:
            return me_w
        base = jnp.where(me_w == W // 2 - 1, 0, W // 2)
        place = (me_w - base + W) % W
        w = (base + step - 1 + jnp.where(step > place, 1, 0)) % W
        return w if isinstance(step, int) else jnp.where(step == 0, me_w, w)

    def word_at(k):
        return k + jnp.where(me_w <= k, 1, 0)

    def sub_at(j):
        if S & (S - 1):
            return (me_s + j) % S
        sub, bit = me_s, 1
        while bit < S:
            sub += (S - 1 - j) // bit % 2 * (1 - me_s // bit % 2 * 2) * bit
            bit *= 2
        return sub

    def load(sem, source, target):
        return pltpu.make_async_copy(source, target, inputs.at[sem])

    first = [
        load(0, tab_hbm.at[me_w], to_ref),
        load(1, desc_hbm, desc_ref),
    ]
    rest = [
        load(2, ids_hbm, ids_ref),
        load(3, wts_hbm, wts_ref),
        load(4, nb_hbm, nb_ref),
        load(5, tab_hbm.at[:, me_w], from_ref),
        load(6, cnt_hbm, cnt_ref),
        load(7, slot_hbm, slot_ref),
    ]
    for copy in first:
        copy.start()

    def words(above, body):
        for_each = lambda k: pl.when((k >= me_w) if above else (k < me_w))(lambda: body(word_at(k)))
        loop(W - 1, 4, for_each)

    def subs(above, body):
        loop(S, 8, lambda s: pl.when((s > me_s) if above else (s < me_s))(lambda: body(s)))

    barrier = pltpu.get_barrier_semaphore()

    def signal(sem, w, s):
        pl.semaphore_signal(sem, inc=1, device_id=(me_g, w, s), device_id_type=MESH)

    subs(True, lambda s: signal(barrier, me_w, s))
    words(True, lambda w: loop(S, 8, lambda s: signal(barrier, w, s)))
    for copy in rest:
        copy.start()
    lower = me_w * S + me_s
    pl.when(lower > 0)(lambda: pl.semaphore_wait(barrier, lower))
    words(False, lambda w: loop(S, 8, lambda s: signal(go.at[me_w], w, s)))
    subs(False, lambda s: signal(go.at[me_w], me_w, s))
    for copy in first:
        copy.wait()

    def pick(slot, w, s):
        for c in range(C):
            outd[slot, c] = desc_ref[to_ref[w, c, s]]

    loop(W - 1, 4, lambda k: loop(S, 8, lambda j: pick(k * S + j, word_at(k), sub_at(j))))
    loop(S, 8, lambda j: pick((W - 1) * S + j, me_w, sub_at(j)))
    for c in range(C):
        held[me_w, me_s, c] = desc_ref[to_ref[me_w, c, me_s]]

    def send(slot, w, s):
        pltpu.make_async_remote_copy(
            src_ref=outd.at[slot], dst_ref=held.at[me_w, me_s],
            send_sem=dsend, recv_sem=drecv.at[me_w],
            device_id=(me_g, w, s), device_id_type=MESH,
        ).start()

    def send_word(k):
        loop(S, 8, lambda j: send(k * S + j, word_at(k), sub_at(j)))

    def send_near(above):
        def each(j):
            s = sub_at(j)
            pl.when((s > me_s) if above else (s < me_s))(lambda: send((W - 1) * S + j, me_w, s))

        loop(S, 8, each)

    pl.when(me_w > 0)(lambda: send_word(0))
    send_near(False)

    for copy in rest:
        copy.wait()

    ids = ids_ref[...]
    table[0:B] = (ids >> 8).astype(F32).astype(BF16)
    table[B : 2 * B] = (ids & 255).astype(F32).astype(BF16)
    for i, piece in enumerate(pieces(wts_ref[...])):
        table[(2 + i) * B : (3 + i) * B] = piece
    nbf[...] = jnp.zeros_like(nbf)
    nbf[0:K] = nb_ref[...]
    near_ids = nbf[...]
    table[TR : TR + KP] = (near_ids >> 8).astype(F32).astype(BF16)
    table[TR + KP : TR + 2 * KP] = (near_ids & 255).astype(F32).astype(BF16)

    chunk = min(I, 256)

    def self_norm(i):
        at = pl.ds(i * chunk if isinstance(i, int) else pl.multiple_of(i * chunk, chunk), chunk)
        here = ids_ref[:, at]
        total = jnp.zeros((B, chunk), F32)
        for a in range(B):
            total += jnp.where(here == ids_ref[a : a + 1, at], wts_ref[a : a + 1, at], F32(0.0))
        norm = jnp.sum(total * wts_ref[:, at], axis=0, keepdims=True)
        row = lax.broadcasted_iota(I32, (16, chunk), 0)
        block = jnp.zeros((16, chunk), F32)
        for k, piece in enumerate(pieces(norm)):
            block = jnp.where(row == k, piece.astype(F32), block)
        table[5 * B : TR, at] = block.astype(BF16)

    loop(I // chunk, 1, self_norm)

    def part_copy(d):
        w = word_at(d)
        return pltpu.make_async_remote_copy(
            src_ref=part_out.at[d], dst_ref=part_in.at[me_w - jnp.where(me_w > w, 1, 0)],
            send_sem=psend, recv_sem=precv,
            device_id=(me_g, w, me_s), device_id_type=MESH,
        )

    early = 2 * me_w < W - 1
    lane = lax.broadcasted_iota(I32, (1, LANES), 1)
    digit = lax.broadcasted_iota(I32, (KK, LANES), 0) == lax.broadcasted_iota(I32, (KK, LANES), 1) // R

    def order(i):
        d = (i + jnp.where(early, me_w, 0)) % max(W - 1, 1)
        if isinstance(i, int):
            return d if i < W - 1 else W - 1
        return jnp.where(i < W - 1, d, W - 1)

    def owned(i):
        d = order(i)
        w = jnp.where(d == W - 1, me_w, word_at(d))
        mine = dot(table[...], onehot((w * S + me_s) * R + lane % R, I))
        own[i, 0:B] = mine[0:B] * 256.0 + mine[B : 2 * B]
        own[i, B : 2 * B] = mine[2 * B : 3 * B] + mine[3 * B : 4 * B] + mine[4 * B : 5 * B]
        own[i, 2 * B : 2 * B + 1] = (
            mine[5 * B : 5 * B + 1] + mine[5 * B + 1 : 5 * B + 2] + mine[5 * B + 2 : 5 * B + 3]
        )
        listed = mine[TR : TR + KP] * 256.0 + mine[TR + KP : TR + 2 * KP]
        for j in range(J):
            chosen = jnp.where(digit, listed[j * KK : (j + 1) * KK], F32(0.0))
            wanted[i, j : j + 1] = jnp.sum(chosen, axis=0, keepdims=True).astype(I32)

    def gather(i):
        got = gots[i % 2] if isinstance(i, int) else gots[0]
        for j in range(J):
            got[:, j * LANES : (j + 1) * LANES] = dot(table[0:TR], onehot(wanted[i, j : j + 1], I))

    def target(i):
        d = order(i)
        got = gots[i % 2] if isinstance(i, int) else gots[0]
        cols = [slice(j * LANES, (j + 1) * LANES) for j in range(J)]
        words_of = [got[0:B, c] * 256.0 + got[B : 2 * B, c] for c in cols]
        total = [jnp.zeros((B, LANES), F32) for c in cols]
        for a in range(B):
            word, weight = own[i, a : a + 1], own[i, B + a : B + a + 1]
            for j in range(J):
                total[j] += jnp.where(words_of[j] == word, weight, F32(0.0))
        for j, c in enumerate(cols):
            values = got[2 * B : 3 * B, c] + got[3 * B : 4 * B, c] + got[4 * B : 5 * B, c]
            part_out[d, j : j + 1] = jnp.sum(total[j] * values, axis=0, keepdims=True)
            norms = got[5 * B : 5 * B + 1, c] + got[5 * B + 1 : 5 * B + 2, c] + got[5 * B + 2 : 5 * B + 3, c]
            part_out[d, J + j : J + j + 1] = norms
        part_out[d, 2 * J : 2 * J + 1] = own[i, 2 * B : 2 * B + 1]

    def far_sends():
        def each(k):
            @pl.when(k >= me_w)
            def _():
                pl.semaphore_wait(go.at[k + 1], S)
                send_word(k)

        loop(W - 1, 4, each)

    def after(i):
        d = order(i)
        if isinstance(i, int) and i == 0:
            pl.when(me_s < S - 1)(lambda: pl.semaphore_wait(go.at[me_w], S - 1 - me_s))
            send_near(True)
            pl.when(jnp.logical_not(early))(far_sends)
        next_high = jnp.logical_and(early, me_w + 1 + i < W)
        pl.when(next_high)(lambda: pl.semaphore_wait(go.at[me_w + 1 + i], S))
        part_copy(d).start()
        pl.when(next_high)(lambda: send_word(d))
        pl.when(jnp.logical_and(jnp.logical_not(early), i + 1 < me_w))(lambda: send_word(me_w - 1 - i))

    loop(W, 4, owned)
    if W <= 4:
        gather(0)
        for i in range(W):
            target(i)
            if i + 1 < W:
                gather(i + 1)
                after(i)
    else:
        def step(i):
            gather(i)
            target(i)

        step(0)
        after(0)
        lax.fori_loop(1, W - 1, lambda i, carry: (step(i), after(i), carry)[2], 0)
        step(W - 1)

    def arrive(i):
        w = turn(i)

        def arrived(slices):
            pltpu.make_async_remote_copy(
                src_ref=held.at[w, pl.ds(0, slices)], dst_ref=held.at[w, pl.ds(0, slices)],
                send_sem=dsend, recv_sem=drecv.at[w],
                device_id=(me_g, me_w, me_s), device_id_type=MESH,
            ).wait_recv()

        if isinstance(i, int):
            arrived(S if i > 0 else S - 1)
        else:
            pl.when(i > 0)(lambda: arrived(S))
            pl.when(i == 0)(lambda: arrived(S - 1))
        for c in range(C):
            h = w * C + c
            full = jnp.concatenate([held[w, s, c] for s in range(S)], axis=0)
            qs[h] = full
            wide = full.astype(F32)
            turned = jnp.transpose(wide)
            rt[h] = (turned * -2.0).astype(BF16)
            count = cnt_ref[w * stored + from_ref[w, c, me_s]]
            down = lax.broadcasted_iota(I32, (width, width), 0)
            square = jnp.sum(turned * turned, axis=1, keepdims=True)
            sqb[h] = jnp.where(down < count, square, F32(1e30))
            flat = jnp.sum(wide * wide, axis=0, keepdims=True)
            live = jnp.where(lax.broadcasted_iota(I32, (8, width), 1) < count, F32(1.0), F32(0.0))
            info[h] = jnp.where(lax.broadcasted_iota(I32, (8, width), 0) == 0, flat, live)

    loop(W - 1, 4, arrive)

    def whole(ref, send_sem, recv_sem):
        return pltpu.make_async_remote_copy(
            src_ref=ref, dst_ref=ref, send_sem=send_sem, recv_sem=recv_sem,
            device_id=(me_g, me_w, me_s), device_id_type=MESH,
        )

    whole(part_in.at[pl.ds(0, W - 1)], psend, precv).wait_recv()
    total = part_out[W - 1]
    for d in range(W - 1):
        total += part_in[d]
    cosine = total[0:J] / jnp.sqrt(total[2 * J : 2 * J + 1] * total[J : 2 * J])
    spread = lax.broadcasted_iota(I32, (R, LANES), 1) % R == lax.broadcasted_iota(I32, (R, LANES), 0)
    out_cols = ceil_to(K, LANES)
    deep = lax.broadcasted_iota(I32, (LANES, out_cols), 0) // R
    across = lax.broadcasted_iota(I32, (LANES, out_cols), 1)
    result = jnp.zeros((R, out_cols), F32)
    for j in range(J):
        place = jnp.where(across == deep + j * KK, F32(1.0), F32(0.0)).astype(BF16)
        for piece in pieces(jnp.where(spread, cosine[j : j + 1], F32(0.0))):
            result += dot(piece, place)
    sim_ref[...] = result[:, 0:K]

    arrive(W - 1)

    pairs = near_ref.shape[0]
    group = 8

    def match(i):
        for k in range(group):
            p = i * group + k
            q, r = slot_ref[0, p], slot_ref[1, p]
            inner = dot(rt[r], qs[q])
            base = sqb[r]
            tops = []
            for t in range(2):
                low = second = None
                for v in range(t, width // 8, 2):
                    x = base[v * 8 : v * 8 + 8] + inner[v * 8 : v * 8 + 8]
                    if low is None:
                        low = x
                    elif second is None:
                        low, second = jnp.minimum(low, x), jnp.maximum(low, x)
                    else:
                        second = jnp.minimum(second, jnp.maximum(low, x))
                        low = jnp.minimum(low, x)
                tops.append((low, second))
            (l0, s0), (l1, s1) = tops
            at = pl.ds(p * 8, 8)
            low_s[at] = jnp.minimum(l0, l1)
            next_s[at] = jnp.minimum(jnp.maximum(l0, l1), jnp.minimum(s0, s1))
            info_s[at] = info[q]

    loop(pairs // group, 4, match)

    rows = [pl.ds(i, pairs, stride=8) for i in range(8)]
    low, second = low_s[rows[0]], next_s[rows[0]]
    for at in rows[1:]:
        l1, s1 = low_s[at], next_s[at]
        second = jnp.minimum(jnp.maximum(low, l1), jnp.minimum(second, s1))
        low = jnp.minimum(low, l1)
    live = info_s[rows[1]] > 0.0
    features = F32(feats * S)
    near_ref[...] = jnp.where(live, (low + info_s[rows[0]]) / features, F32(0.0))
    marg_ref[...] = jnp.where(live, (second - low) / features, F32(0.0))

    whole(outd.at[pl.ds(0, n - 1)], dsend, drecv.at[0]).wait_send()
    whole(part_out.at[pl.ds(0, W - 1)], psend, precv).wait_send()


def finish(*refs):
    sems = refs[6]
    copies = [pltpu.make_async_copy(refs[i], refs[3 + i], sems.at[i]) for i in range(3)]
    for copy in copies:
        copy.start()
    for copy in copies:
        copy.wait()


def local(W, S, word_ids, word_weights, neighbours, descriptors, keypoint_count, send_table, pair_slots):
    B, I = word_ids.shape[1:]
    K = neighbours.shape[0]
    R = I // (W * S)
    KK = LANES // R
    J = -(-K // KK)
    C = send_table.shape[-1]
    TR = ceil_to(5 * B + 3, 16)
    KP = ceil_to(J * KK, 16)
    NP = ceil_to(2 * J + 1, 8)
    H = W * C
    stored, feats, width = descriptors.shape
    pairs = pair_slots.shape[2]
    vmem = pl.BlockSpec(memory_space=pltpu.VMEM)
    results = ((R, K), (pairs, width), (pairs, width))
    parts = pl.pallas_call(
        functools.partial(kernel, W, S, (B, I, K, R, KK, J, C, TR, KP, NP, H)),
        out_shape=tuple(pltpu.VMEM(shape, F32) for shape in results),
        in_specs=[pl.BlockSpec(memory_space=pltpu.HBM)] * 7,
        out_specs=(vmem, vmem, vmem),
        scratch_shapes=[
            pltpu.VMEM((B, I), I32),
            pltpu.VMEM((B, I), F32),
            pltpu.VMEM((K, I), I32),
            pltpu.VMEM(descriptors.shape, BF16),
            pltpu.SMEM(keypoint_count.shape, I32),
            pltpu.SMEM((W, C, S), I32),
            pltpu.SMEM((W, C, S), I32),
            pltpu.SMEM((2, pairs), I32),
            pltpu.VMEM((W * S, C, feats, width), BF16),
            pltpu.VMEM((W, S, C, feats, width), BF16),
            pltpu.VMEM((TR + 2 * KP, I), BF16),
            pltpu.VMEM((KP, I), I32),
            pltpu.VMEM((W, 2 * B + 8, LANES), F32),
            pltpu.VMEM((W, ceil_to(J, 8), LANES), I32),
            pltpu.VMEM((TR, J * LANES), F32),
            pltpu.VMEM((TR, J * LANES), F32),
            pltpu.VMEM((W, NP, LANES), F32),
            pltpu.VMEM((W, NP, LANES), F32),
            pltpu.VMEM((H, width, width), BF16),
            pltpu.VMEM((H, width, width), BF16),
            pltpu.VMEM((H, width, width), F32),
            pltpu.VMEM((H, 8, width), F32),
            pltpu.VMEM((pairs * 8, width), F32),
            pltpu.VMEM((pairs * 8, width), F32),
            pltpu.VMEM((pairs * 8, width), F32),
            pltpu.SemaphoreType.DMA,
            pltpu.SemaphoreType.DMA((W,)),
            pltpu.SemaphoreType.DMA,
            pltpu.SemaphoreType.DMA,
            pltpu.SemaphoreType.DMA((8,)),
            pltpu.SemaphoreType.REGULAR((W,)),
        ],
        compiler_params=pltpu.CompilerParams(
            collective_id=0, has_side_effects=True, vmem_limit_bytes=LIMIT
        ),
    )(*(pltpu.with_memory_space_constraint(operand, pltpu.HBM) for operand in (
        word_ids[0], word_weights[0], neighbours, descriptors,
        keypoint_count, jnp.swapaxes(send_table, 2, 3), jnp.swapaxes(pair_slots, 2, 3)[0, 0],
    )))
    similarity, nearest, margin = pl.pallas_call(
        finish,
        out_shape=tuple(jax.ShapeDtypeStruct(shape, F32) for shape in results),
        in_specs=[pl.BlockSpec(memory_space=pl.ANY)] * 3,
        out_specs=(pl.BlockSpec(memory_space=pltpu.HBM),) * 3,
        scratch_shapes=[pltpu.SemaphoreType.DMA((3,))],
        compiler_params=pltpu.CompilerParams(vmem_limit_bytes=LIMIT),
    )(*parts)
    return similarity, nearest[None, None], margin[None, None]


def solution(mesh):
    in_specs = (
        P("word", None, "groups"),
        P("word", None, "groups"),
        P(None, "groups"),
        P(("groups", "word"), "sub", None),
        P("groups"),
        P("groups", None, None, None),
        P(("groups", "word"), "sub", None, None),
    )
    out_specs = (
        P(("groups", "word", "sub"), None),
        P(("groups", "word"), "sub", None, None),
        P(("groups", "word"), "sub", None, None),
    )
    body = functools.partial(local, mesh.shape["word"], mesh.shape["sub"])
    return jax.shard_map(body, mesh=mesh, in_specs=in_specs, out_specs=out_specs, check_vma=False)
```

```python
import functools

import jax
import jax.numpy as jnp
from jax import lax
from jax.experimental import pallas as pl
from jax.experimental.pallas import tpu as pltpu
from jax.sharding import PartitionSpec as P

MESH = pl.DeviceIdType.MESH
LANES = 128
LIMIT = 40 * 1024 * 1024
F32, BF16, I32 = jnp.float32, jnp.bfloat16, jnp.int32


def ceil_to(value, step):
    return (value + step - 1) // step * step


def loop(count, limit, body):
    if count <= limit:
        for i in range(count):
            body(i)
    else:
        lax.fori_loop(0, count, lambda i, carry: (body(i), carry)[1], 0)


def pieces(x):
    first = x.astype(BF16)
    return first, (x - first.astype(F32)).astype(BF16)


def dot(a, b):
    return lax.dot_general(a, b, (((1,), (0,)), ((), ())), preferred_element_type=F32)


def onehot(want, rows):
    numbers = lax.broadcasted_iota(I32, (rows, want.shape[-1]), 0)
    return jnp.where(numbers == want, F32(1.0), F32(0.0)).astype(BF16)


def kernel(
    W, S, dims,
    ids_hbm, wts_hbm, nb_hbm, desc_hbm, cnt_hbm, tab_hbm, slot_hbm,
    sim_ref, near_ref, marg_ref,
    ids_ref, wts_ref, nb_ref, desc_ref, cnt_ref, to_ref, from_ref, slot_ref,
    outd, held, table, nbf, own, wanted, got_0, got_1, part_out, part_in,
    qs, rt, sqb, info, low_t, next_t, low_s, next_s, info_s,
    dsend, drecv, psend, precv, inputs, go,
):
    B, I, K, R, KK, J, C, TR, KP, NP, H = dims
    gots = got_0, got_1
    gram = qs.shape[0] == W
    me_g, me_w, me_s = lax.axis_index("groups"), lax.axis_index("word"), lax.axis_index("sub")
    n = W * S
    stored, feats, width = desc_ref.shape

    def turn(step):
        if isinstance(step, int) and step == 0:
            return me_w
        inner = early
        place = jnp.where(inner, W - me_w, me_w + W - W // 2) % W
        k = step - 1 + jnp.where(step > place, 1, 0)
        w = jnp.where(inner, W - k, W // 2 + k) % W
        return w if isinstance(step, int) else jnp.where(step == 0, me_w, w)

    def word_at(k):
        return k + jnp.where(me_w <= k, 1, 0)

    def sub_at(j):
        if S & (S - 1):
            return (me_s + j) % S
        sub, bit = me_s, 1
        while bit < S:
            sub += (S - 1 - j) // bit % 2 * (1 - me_s // bit % 2 * 2) * bit
            bit *= 2
        return sub

    def load(sem, source, target):
        return pltpu.make_async_copy(source, target, inputs.at[sem])

    first = [
        load(0, tab_hbm.at[me_w], to_ref),
        load(0, desc_hbm, desc_ref),
    ]
    rest = [
        load(1, ids_hbm, ids_ref),
        load(1, wts_hbm, wts_ref),
        load(1, nb_hbm, nb_ref),
        load(1, tab_hbm.at[:, me_w], from_ref),
        load(1, cnt_hbm, cnt_ref),
        load(1, slot_hbm, slot_ref),
    ]
    for copy in first:
        copy.start()

    def words(above, body):
        for_each = lambda k: pl.when((k >= me_w) if above else (k < me_w))(lambda: body(word_at(k)))
        loop(W - 1, 4, for_each)

    def subs(above, body):
        loop(S, 8, lambda s: pl.when((s > me_s) if above else (s < me_s))(lambda: body(s)))

    barrier = pltpu.get_barrier_semaphore()

    def signal(sem, w, s):
        pl.semaphore_signal(sem, inc=1, device_id=(me_g, w, s), device_id_type=MESH)

    subs(True, lambda s: signal(barrier, me_w, s))
    words(True, lambda w: loop(S, 8, lambda s: signal(barrier, w, s)))
    for copy in rest:
        copy.start()
    lower = me_w * S + me_s
    pl.when(lower > 0)(lambda: pl.semaphore_wait(barrier, lower))
    words(False, lambda w: loop(S, 8, lambda s: signal(go.at[me_w], w, s)))
    subs(False, lambda s: signal(go.at[me_w], me_w, s))
    for copy in first:
        copy.wait()

    def pick(slot, w, s):
        for c in range(C):
            outd[slot, c] = desc_ref[to_ref[w, c, s]]

    loop(W - 1, 4, lambda k: loop(S, 8, lambda j: pick(k * S + j, word_at(k), sub_at(j))))
    loop(S, 8, lambda j: pick((W - 1) * S + j, me_w, sub_at(j)))
    for c in range(C):
        held[me_w, me_s, c] = desc_ref[to_ref[me_w, c, me_s]]

    def send(slot, w, s):
        pltpu.make_async_remote_copy(
            src_ref=outd.at[slot], dst_ref=held.at[me_w, me_s],
            send_sem=dsend, recv_sem=drecv.at[me_w],
            device_id=(me_g, w, s), device_id_type=MESH,
        ).start()

    def send_word(k):
        loop(S, 8, lambda j: send(k * S + j, word_at(k), sub_at(j)))

    def send_near(above):
        def each(j):
            s = sub_at(j)
            pl.when((s > me_s) if above else (s < me_s))(lambda: send((W - 1) * S + j, me_w, s))

        loop(S, 8, each)

    early = 2 * me_w < W - 1
    late = jnp.logical_not(early)
    pl.when(me_w > 0)(lambda: send_word(0))
    send_near(False)

    for copy in rest:
        copy.wait()

    ids = ids_ref[...]
    table[0:B] = (ids >> 8).astype(F32).astype(BF16)
    table[B : 2 * B] = (ids & 255).astype(F32).astype(BF16)
    for i, piece in enumerate(pieces(wts_ref[...])):
        table[(2 + i) * B : (3 + i) * B] = piece
    nbf[...] = jnp.zeros_like(nbf)
    nbf[0:K] = nb_ref[...]
    near_ids = nbf[...]
    table[TR : TR + KP] = (near_ids >> 8).astype(F32).astype(BF16)
    table[TR + KP : TR + 2 * KP] = (near_ids & 255).astype(F32).astype(BF16)

    chunk = min(I, 256)

    def self_norm(i):
        at = pl.ds(i * chunk if isinstance(i, int) else pl.multiple_of(i * chunk, chunk), chunk)
        here = ids_ref[:, at]
        total = jnp.zeros((B, chunk), F32)
        for a in range(B):
            total += jnp.where(here == ids_ref[a : a + 1, at], wts_ref[a : a + 1, at], F32(0.0))
        norm = jnp.sum(total * wts_ref[:, at], axis=0, keepdims=True)
        row = lax.broadcasted_iota(I32, (16, chunk), 0)
        block = jnp.zeros((16, chunk), F32)
        for k, piece in enumerate(pieces(norm)):
            block = jnp.where(row == k, piece.astype(F32), block)
        table[4 * B : TR, at] = block.astype(BF16)

    loop(I // chunk, 1, self_norm)

    def part_copy(d):
        w = word_at(d)
        return pltpu.make_async_remote_copy(
            src_ref=part_out.at[d], dst_ref=part_in.at[me_w - jnp.where(me_w > w, 1, 0)],
            send_sem=psend, recv_sem=precv,
            device_id=(me_g, w, me_s), device_id_type=MESH,
        )

    lane = lax.broadcasted_iota(I32, (1, LANES), 1)
    digit = lax.broadcasted_iota(I32, (KK, LANES), 0) == lax.broadcasted_iota(I32, (KK, LANES), 1) // R

    def order(i):
        d = (i + jnp.where(early, me_w, 0)) % max(W - 1, 1)
        if isinstance(i, int):
            return d if i < W - 1 else W - 1
        return jnp.where(i < W - 1, d, W - 1)

    def owned(i):
        d = order(i)
        w = jnp.where(d == W - 1, me_w, word_at(d))
        mine = dot(table[...], onehot((w * S + me_s) * R + lane % R, I))
        own[i, 0:B] = mine[0:B] * 256.0 + mine[B : 2 * B]
        own[i, B : 2 * B] = mine[2 * B : 3 * B] + mine[3 * B : 4 * B]
        own[i, 2 * B : 2 * B + 1] = mine[4 * B : 4 * B + 1] + mine[4 * B + 1 : 4 * B + 2]
        listed = mine[TR : TR + KP] * 256.0 + mine[TR + KP : TR + 2 * KP]
        for j in range(J):
            chosen = jnp.where(digit, listed[j * KK : (j + 1) * KK], F32(0.0))
            wanted[i, j : j + 1] = jnp.sum(chosen, axis=0, keepdims=True).astype(I32)

    def gather(i):
        got = gots[i % 2] if isinstance(i, int) else gots[0]
        for j in range(J):
            got[:, j * LANES : (j + 1) * LANES] = dot(table[0:TR], onehot(wanted[i, j : j + 1], I))

    def target(i):
        d = order(i)
        got = gots[i % 2] if isinstance(i, int) else gots[0]
        cols = [slice(j * LANES, (j + 1) * LANES) for j in range(J)]
        words_of = [got[0:B, c] * 256.0 + got[B : 2 * B, c] for c in cols]
        total = [jnp.zeros((B, LANES), F32) for c in cols]
        for a in range(B):
            word, weight = own[i, a : a + 1], own[i, B + a : B + a + 1]
            for j in range(J):
                total[j] += jnp.where(words_of[j] == word, weight, F32(0.0))
        for j, c in enumerate(cols):
            values = got[2 * B : 3 * B, c] + got[3 * B : 4 * B, c]
            part_out[d, j : j + 1] = jnp.sum(total[j] * values, axis=0, keepdims=True)
            norms = got[4 * B : 4 * B + 1, c] + got[4 * B + 1 : 4 * B + 2, c]
            part_out[d, J + j : J + j + 1] = norms
        part_out[d, 2 * J : 2 * J + 1] = own[i, 2 * B : 2 * B + 1]

    def far_sends():
        def each(k):
            @pl.when(k >= me_w)
            def _():
                pl.semaphore_wait(go.at[k + 1], S)
                send_word(k)

        loop(W - 1, 4, each)

    def after(i):
        d = order(i)
        if isinstance(i, int) and i == 0:
            pl.when(me_s < S - 1)(lambda: pl.semaphore_wait(go.at[me_w], S - 1 - me_s))
            send_near(True)
            pl.when(late)(far_sends)
        high = me_w + 1 + i < W
        wait_high = jnp.logical_and(early, high)
        pl.when(wait_high)(lambda: pl.semaphore_wait(go.at[me_w + 1 + i], S))
        part_copy(d).start()
        pl.when(wait_high)(lambda: send_word(d))
        rest_low = jnp.logical_and(jnp.logical_and(early, jnp.logical_not(high)), d > 0)
        pl.when(rest_low)(lambda: send_word(d))
        if isinstance(i, int) and i == 0:
            pl.when(jnp.logical_and(late, me_w > 2))(lambda: send_word(me_w - 1))
        else:
            held_back = jnp.logical_or(i < me_w - 1, jnp.logical_and(i == 1, me_w == 2))
            pl.when(jnp.logical_and(late, held_back))(lambda: send_word(i))

    loop(W, 4, owned)
    if W <= 4:
        gather(0)
        for i in range(W):
            target(i)
            if i + 1 < W:
                gather(i + 1)
                after(i)
    else:
        def step(i):
            gather(i)
            target(i)

        step(0)
        after(0)
        lax.fori_loop(1, W - 1, lambda i, carry: (step(i), after(i), carry)[2], 0)
        step(W - 1)

    pairs = near_ref.shape[0]
    group = 8

    order_of = [turn(i) for i in range(W)] if gram else None

    def lowest_two(base, inner):
        tops = []
        for t in range(2):
            low = second = None
            for v in range(t, width // 8, 2):
                x = base[v * 8 : v * 8 + 8] + inner[v * 8 : v * 8 + 8]
                if low is None:
                    low = x
                elif second is None:
                    low, second = jnp.minimum(low, x), jnp.maximum(low, x)
                else:
                    second = jnp.minimum(second, jnp.maximum(low, x))
                    low = jnp.minimum(low, x)
            tops.append((low, second))
        (l0, s0), (l1, s1) = tops
        return jnp.minimum(l0, l1), jnp.minimum(jnp.maximum(l0, l1), jnp.minimum(s0, s1))

    def block(j, b):
        inner = dot(rt[b], qs[j])
        base = sqb[b]
        for c in range(C):
            a = j * C + c
            if a != b:
                cell = (order_of[j] * C + c) * H + order_of[b // C] * C + b % C
                low_t[cell], next_t[cell] = lowest_two(base, inner[:, c * width : (c + 1) * width])

    def arrive(i):
        w = order_of[i] if gram else turn(i)

        def arrived(slices):
            pltpu.make_async_remote_copy(
                src_ref=held.at[w, pl.ds(0, slices)], dst_ref=held.at[w, pl.ds(0, slices)],
                send_sem=dsend, recv_sem=drecv.at[w],
                device_id=(me_g, me_w, me_s), device_id_type=MESH,
            ).wait_recv()

        if isinstance(i, int):
            arrived(S if i > 0 else S - 1)
        else:
            pl.when(i > 0)(lambda: arrived(S))
            pl.when(i == 0)(lambda: arrived(S - 1))
        for c in range(C):
            h = i * C + c if gram else w * C + c
            full = jnp.concatenate([held[w, s, c] for s in range(S)], axis=0)
            if gram:
                qs[i, :, c * width : (c + 1) * width] = full
            else:
                qs[h] = full
            wide = full.astype(F32)
            turned = jnp.transpose(wide)
            rt[h] = (turned * -2.0).astype(BF16)
            count = cnt_ref[w * stored + from_ref[w, c, me_s]]
            down = lax.broadcasted_iota(I32, (width, width), 0)
            square = jnp.sum(turned * turned, axis=1, keepdims=True)
            sqb[h] = jnp.where(down < count, square, F32(1e30))
            flat = jnp.sum(wide * wide, axis=0, keepdims=True)
            live = jnp.where(lax.broadcasted_iota(I32, (8, width), 1) < count, F32(1.0), F32(0.0))
            info[w * C + c] = jnp.where(lax.broadcasted_iota(I32, (8, width), 0) == 0, flat, live)
        if gram:
            for b in range((i + 1) * C):
                block(i, b)
            for j in range(i):
                for c in range(C):
                    block(j, i * C + c)

    def whole(ref, send_sem, recv_sem):
        return pltpu.make_async_remote_copy(
            src_ref=ref, dst_ref=ref, send_sem=send_sem, recv_sem=recv_sem,
            device_id=(me_g, me_w, me_s), device_id_type=MESH,
        )

    def similarity():
        whole(part_in.at[pl.ds(0, W - 1)], psend, precv).wait_recv()
        total = part_out[W - 1]
        for d in range(W - 1):
            total += part_in[d]
        cosine = total[0:J] / jnp.sqrt(total[2 * J : 2 * J + 1] * total[J : 2 * J])
        spread = lax.broadcasted_iota(I32, (R, LANES), 1) % R == lax.broadcasted_iota(I32, (R, LANES), 0)
        out_cols = ceil_to(K, LANES)
        deep = lax.broadcasted_iota(I32, (LANES, out_cols), 0) // R
        across = lax.broadcasted_iota(I32, (LANES, out_cols), 1)
        result = jnp.zeros((R, out_cols), F32)
        for j in range(J):
            place = jnp.where(across == deep + j * KK, F32(1.0), F32(0.0)).astype(BF16)
            for piece in pieces(jnp.where(spread, cosine[j : j + 1], F32(0.0))):
                result += dot(piece, place)
        sim_ref[...] = result[:, 0:K]

    if 2 < W <= 4:
        arrive(0)
        arrive(1)
        pl.when(me_w == 0)(similarity)
        loop(W - 3, 4, lambda i: arrive(2 + i))
        pl.when(me_w > 0)(similarity)
    else:
        loop(W - 1, 4, arrive)
        similarity()
    arrive(W - 1)

    def match(i):
        for k in range(group):
            p = i * group + k
            a, b = slot_ref[0, p], slot_ref[1, p]
            at = pl.ds(p * 8, 8)
            if gram:
                low_s[at], next_s[at] = low_t[a * H + b], next_t[a * H + b]
            else:
                low_s[at], next_s[at] = lowest_two(sqb[b], dot(rt[b], qs[a]))
            info_s[at] = info[a]

    loop(pairs // group, 4, match)

    rows = [pl.ds(i, pairs, stride=8) for i in range(8)]
    low, second = low_s[rows[0]], next_s[rows[0]]
    for at in rows[1:]:
        l1, s1 = low_s[at], next_s[at]
        second = jnp.minimum(jnp.maximum(low, l1), jnp.minimum(second, s1))
        low = jnp.minimum(low, l1)
    live = info_s[rows[1]] > 0.0
    features = F32(feats * S)
    near_ref[...] = jnp.where(live, (low + info_s[rows[0]]) / features, F32(0.0))
    marg_ref[...] = jnp.where(live, (second - low) / features, F32(0.0))

    whole(outd.at[pl.ds(0, n - 1)], dsend, drecv.at[0]).wait_send()
    whole(part_out.at[pl.ds(0, W - 1)], psend, precv).wait_send()


def finish(*refs):
    sems = refs[6]
    copies = [pltpu.make_async_copy(refs[i], refs[3 + i], sems.at[i]) for i in range(3)]
    for copy in copies:
        copy.start()
    for copy in copies:
        copy.wait()


def local(W, S, word_ids, word_weights, neighbours, descriptors, keypoint_count, send_table, pair_slots):
    B, I = word_ids.shape[1:]
    K = neighbours.shape[0]
    R = I // (W * S)
    KK = LANES // R
    J = -(-K // KK)
    C = send_table.shape[-1]
    TR = ceil_to(4 * B + 2, 16)
    KP = ceil_to(J * KK, 16)
    NP = ceil_to(2 * J + 1, 8)
    H = W * C
    stored, feats, width = descriptors.shape
    pairs = pair_slots.shape[2]
    gram = W <= 4 and C > 1 and H * H <= 2 * pairs
    vmem = pl.BlockSpec(memory_space=pltpu.VMEM)
    results = ((R, K), (pairs, width), (pairs, width))
    parts = pl.pallas_call(
        functools.partial(kernel, W, S, (B, I, K, R, KK, J, C, TR, KP, NP, H)),
        out_shape=tuple(pltpu.VMEM(shape, F32) for shape in results),
        in_specs=[pl.BlockSpec(memory_space=pltpu.HBM)] * 7,
        out_specs=(vmem, vmem, vmem),
        scratch_shapes=[
            pltpu.VMEM((B, I), I32),
            pltpu.VMEM((B, I), F32),
            pltpu.VMEM((K, I), I32),
            pltpu.VMEM(descriptors.shape, BF16),
            pltpu.SMEM(keypoint_count.shape, I32),
            pltpu.SMEM((W, C, S), I32),
            pltpu.SMEM((W, C, S), I32),
            pltpu.SMEM((2, pairs), I32),
            pltpu.VMEM((W * S, C, feats, width), BF16),
            pltpu.VMEM((W, S, C, feats, width), BF16),
            pltpu.VMEM((TR + 2 * KP, I), BF16),
            pltpu.VMEM((KP, I), I32),
            pltpu.VMEM((W, 2 * B + 8, LANES), F32),
            pltpu.VMEM((W, ceil_to(J, 8), LANES), I32),
            pltpu.VMEM((TR, J * LANES), F32),
            pltpu.VMEM((TR, J * LANES), F32),
            pltpu.VMEM((W, NP, LANES), F32),
            pltpu.VMEM((W, NP, LANES), F32),
            pltpu.VMEM((W, width, C * width) if gram else (H, width, width), BF16),
            pltpu.VMEM((H, width, width), BF16),
            pltpu.VMEM((H, width, width), F32),
            pltpu.VMEM((H, 8, width), F32),
            pltpu.VMEM((H * H if gram else 1, 8, width), F32),
            pltpu.VMEM((H * H if gram else 1, 8, width), F32),
            pltpu.VMEM((pairs * 8, width), F32),
            pltpu.VMEM((pairs * 8, width), F32),
            pltpu.VMEM((pairs * 8, width), F32),
            pltpu.SemaphoreType.DMA,
            pltpu.SemaphoreType.DMA((W,)),
            pltpu.SemaphoreType.DMA,
            pltpu.SemaphoreType.DMA,
            pltpu.SemaphoreType.DMA((2,)),
            pltpu.SemaphoreType.REGULAR((W,)),
        ],
        compiler_params=pltpu.CompilerParams(
            collective_id=0, has_side_effects=True, vmem_limit_bytes=LIMIT
        ),
    )(*(pltpu.with_memory_space_constraint(operand, pltpu.HBM) for operand in (
        word_ids[0], word_weights[0], neighbours, descriptors,
        keypoint_count, jnp.swapaxes(send_table, 2, 3), jnp.swapaxes(pair_slots, 2, 3)[0, 0],
    )))
    similarity, nearest, margin = pl.pallas_call(
        finish,
        out_shape=tuple(jax.ShapeDtypeStruct(shape, F32) for shape in results),
        in_specs=[pl.BlockSpec(memory_space=pl.ANY)] * 3,
        out_specs=(pl.BlockSpec(memory_space=pltpu.HBM),) * 3,
        scratch_shapes=[pltpu.SemaphoreType.DMA((3,))],
        compiler_params=pltpu.CompilerParams(vmem_limit_bytes=LIMIT),
    )(*parts)
    return similarity, nearest[None, None], margin[None, None]


def solution(mesh):
    in_specs = (
        P("word", None, "groups"),
        P("word", None, "groups"),
        P(None, "groups"),
        P(("groups", "word"), "sub", None),
        P("groups"),
        P("groups", None, None, None),
        P(("groups", "word"), "sub", None, None),
    )
    out_specs = (
        P(("groups", "word", "sub"), None),
        P(("groups", "word"), "sub", None, None),
        P(("groups", "word"), "sub", None, None),
    )
    body = functools.partial(local, mesh.shape["word"], mesh.shape["sub"])
    return jax.shard_map(body, mesh=mesh, in_specs=in_specs, out_specs=out_specs, check_vma=False)
```

```python
import functools

import jax
import jax.numpy as jnp
from jax import lax
from jax.experimental import pallas as pl
from jax.experimental.pallas import tpu as pltpu
from jax.sharding import PartitionSpec as P

MESH = pl.DeviceIdType.MESH
LANES = 128
LIMIT = 40 * 1024 * 1024
F32, BF16, I32 = jnp.float32, jnp.bfloat16, jnp.int32


def ceil_to(value, step):
    return (value + step - 1) // step * step


def loop(count, limit, body):
    if count <= limit:
        for i in range(count):
            body(i)
    else:
        lax.fori_loop(0, count, lambda i, carry: (body(i), carry)[1], 0)


def pieces(x):
    first = x.astype(BF16)
    return first, (x - first.astype(F32)).astype(BF16)


def dot(a, b):
    return lax.dot_general(a, b, (((1,), (0,)), ((), ())), preferred_element_type=F32)


def onehot(want, rows):
    numbers = lax.broadcasted_iota(I32, (rows, want.shape[-1]), 0)
    return jnp.where(numbers == want, F32(1.0), F32(0.0)).astype(BF16)


def kernel(
    W, S, dims,
    ids_hbm, wts_hbm, nb_hbm, desc_hbm, cnt_hbm, tab_hbm, slot_hbm,
    sim_ref, near_ref, marg_ref,
    ids_ref, wts_ref, nb_ref, desc_ref, cnt_ref, to_ref, from_ref, slot_ref,
    outd, held, table, nbf, own, wanted, got_0, got_1, part_out, part_in,
    qs, rt, sqb, info, low_t, next_t, low_s, next_s, info_s,
    dsend, drecv, psend, precv, inputs, go,
):
    B, I, K, R, KK, J, C, TR, KP, NP, H = dims
    gots = got_0, got_1
    gram = qs.shape[0] == W
    me_g, me_w, me_s = lax.axis_index("groups"), lax.axis_index("word"), lax.axis_index("sub")
    n = W * S
    stored, feats, width = desc_ref.shape

    def turn(step):
        if isinstance(step, int) and step == 0:
            return me_w
        inner = early
        place = jnp.where(inner, W - me_w, me_w + W - W // 2) % W
        k = step - 1 + jnp.where(step > place, 1, 0)
        w = jnp.where(inner, W - k, W // 2 + k) % W
        return w if isinstance(step, int) else jnp.where(step == 0, me_w, w)

    def word_at(k):
        return k + jnp.where(me_w <= k, 1, 0)

    def sub_at(j):
        if S & (S - 1):
            return (me_s + j) % S
        sub, bit = me_s, 1
        while bit < S:
            sub += (S - 1 - j) // bit % 2 * (1 - me_s // bit % 2 * 2) * bit
            bit *= 2
        return sub

    def load(sem, source, target):
        return pltpu.make_async_copy(source, target, inputs.at[sem])

    first = [
        load(0, tab_hbm.at[me_w], to_ref),
        load(0, desc_hbm, desc_ref),
    ]
    rest = [
        load(1, ids_hbm, ids_ref),
        load(1, wts_hbm, wts_ref),
        load(1, nb_hbm, nb_ref),
        load(1, tab_hbm.at[:, me_w], from_ref),
        load(1, cnt_hbm, cnt_ref),
        load(1, slot_hbm, slot_ref),
    ]
    for copy in first:
        copy.start()

    def words(above, body):
        for_each = lambda k: pl.when((k >= me_w) if above else (k < me_w))(lambda: body(word_at(k)))
        loop(W - 1, 4, for_each)

    def subs(above, body):
        loop(S, 8, lambda s: pl.when((s > me_s) if above else (s < me_s))(lambda: body(s)))

    barrier = pltpu.get_barrier_semaphore()

    def signal(sem, w, s):
        pl.semaphore_signal(sem, inc=1, device_id=(me_g, w, s), device_id_type=MESH)

    half, mid = S // 2, W // 2
    paired = W > 1 and S > 1 and not W & (W - 1) and not S & (S - 1)
    below, above = jnp.logical_and(paired, me_w == mid - 1), jnp.logical_and(paired, me_w == mid)
    side = me_s // max(half, 1) * half

    subs(True, lambda s: signal(barrier, me_w, s))
    if paired:
        pl.when(above)(lambda: loop(half, 8, lambda j: signal(barrier, mid - 1, side + j)))
    words(True, lambda w: loop(S, 8, lambda s: signal(barrier, w, s)))
    for copy in rest:
        copy.start()
    lower = me_w * S + me_s + jnp.where(below, half, 0)
    pl.when(lower > 0)(lambda: pl.semaphore_wait(barrier, lower))
    def answer(w):
        mate = jnp.logical_and(above, w == mid - 1)
        if paired:
            pl.when(mate)(lambda: loop(half, 8, lambda j: signal(go.at[me_w], w, half - side + j)))
        pl.when(jnp.logical_not(mate))(lambda: loop(S, 8, lambda s: signal(go.at[me_w], w, s)))

    words(False, answer)
    subs(False, lambda s: signal(go.at[me_w], me_w, s))
    for copy in first:
        copy.wait()

    def pick(slot, w, s):
        for c in range(C):
            outd[slot, c] = desc_ref[to_ref[w, c, s]]

    loop(W - 1, 4, lambda k: loop(S, 8, lambda j: pick(k * S + j, word_at(k), sub_at(j))))
    loop(S, 8, lambda j: pick((W - 1) * S + j, me_w, sub_at(j)))
    for c in range(C):
        held[me_w, me_s, c] = desc_ref[to_ref[me_w, c, me_s]]

    def send(slot, w, s):
        pltpu.make_async_remote_copy(
            src_ref=outd.at[slot], dst_ref=held.at[me_w, me_s],
            send_sem=dsend, recv_sem=drecv.at[me_w],
            device_id=(me_g, w, s), device_id_type=MESH,
        ).start()

    def send_word(k, first=0, last=S):
        loop(last - first, 8, lambda j: send(k * S + first + j, word_at(k), sub_at(first + j)))

    def send_near(above):
        def each(j):
            s = sub_at(j)
            pl.when((s > me_s) if above else (s < me_s))(lambda: send((W - 1) * S + j, me_w, s))

        loop(S, 8, each)

    early = 2 * me_w < W - 1
    late = jnp.logical_not(early)
    left = me_s < half
    if paired:
        pl.when(below)(lambda: send_word(mid - 1, half, S))
    pl.when(jnp.logical_and(me_w > 0, left))(lambda: send_word(0, half, S))
    pl.when(me_w > 0)(lambda: send_word(0, 0, half))
    pl.when(jnp.logical_and(me_w > 0, jnp.logical_not(left)))(lambda: send_word(0, half, S))
    send_near(False)

    for copy in rest:
        copy.wait()

    ids = ids_ref[...]
    table[0:B] = (ids >> 8).astype(F32).astype(BF16)
    table[B : 2 * B] = (ids & 255).astype(F32).astype(BF16)
    for i, piece in enumerate(pieces(wts_ref[...])):
        table[(2 + i) * B : (3 + i) * B] = piece
    nbf[...] = jnp.zeros_like(nbf)
    nbf[0:K] = nb_ref[...]
    near_ids = nbf[...]
    table[TR : TR + KP] = (near_ids >> 8).astype(F32).astype(BF16)
    table[TR + KP : TR + 2 * KP] = (near_ids & 255).astype(F32).astype(BF16)

    chunk = min(I, 256)

    def self_norm(i):
        at = pl.ds(i * chunk if isinstance(i, int) else pl.multiple_of(i * chunk, chunk), chunk)
        here = ids_ref[:, at]
        total = jnp.zeros((B, chunk), F32)
        for a in range(B):
            total += jnp.where(here == ids_ref[a : a + 1, at], wts_ref[a : a + 1, at], F32(0.0))
        norm = jnp.sum(total * wts_ref[:, at], axis=0, keepdims=True)
        row = lax.broadcasted_iota(I32, (16, chunk), 0)
        block = jnp.zeros((16, chunk), F32)
        for k, piece in enumerate(pieces(norm)):
            block = jnp.where(row == k, piece.astype(F32), block)
        table[4 * B : TR, at] = block.astype(BF16)

    loop(I // chunk, 1, self_norm)

    def part_copy(d):
        w = word_at(d)
        return pltpu.make_async_remote_copy(
            src_ref=part_out.at[d], dst_ref=part_in.at[me_w - jnp.where(me_w > w, 1, 0)],
            send_sem=psend, recv_sem=precv,
            device_id=(me_g, w, me_s), device_id_type=MESH,
        )

    lane = lax.broadcasted_iota(I32, (1, LANES), 1)
    digit = lax.broadcasted_iota(I32, (KK, LANES), 0) == lax.broadcasted_iota(I32, (KK, LANES), 1) // R

    def order(i):
        d = (i + jnp.where(early, me_w, 0)) % max(W - 1, 1)
        if isinstance(i, int):
            return d if i < W - 1 else W - 1
        return jnp.where(i < W - 1, d, W - 1)

    def owned(i):
        d = order(i)
        w = jnp.where(d == W - 1, me_w, word_at(d))
        mine = dot(table[...], onehot((w * S + me_s) * R + lane % R, I))
        own[i, 0:B] = mine[0:B] * 256.0 + mine[B : 2 * B]
        own[i, B : 2 * B] = mine[2 * B : 3 * B] + mine[3 * B : 4 * B]
        own[i, 2 * B : 2 * B + 1] = mine[4 * B : 4 * B + 1] + mine[4 * B + 1 : 4 * B + 2]
        listed = mine[TR : TR + KP] * 256.0 + mine[TR + KP : TR + 2 * KP]
        for j in range(J):
            chosen = jnp.where(digit, listed[j * KK : (j + 1) * KK], F32(0.0))
            wanted[i, j : j + 1] = jnp.sum(chosen, axis=0, keepdims=True).astype(I32)

    def gather(i):
        got = gots[i % 2] if isinstance(i, int) else gots[0]
        for j in range(J):
            got[:, j * LANES : (j + 1) * LANES] = dot(table[0:TR], onehot(wanted[i, j : j + 1], I))

    def target(i):
        d = order(i)
        got = gots[i % 2] if isinstance(i, int) else gots[0]
        cols = [slice(j * LANES, (j + 1) * LANES) for j in range(J)]
        words_of = [got[0:B, c] * 256.0 + got[B : 2 * B, c] for c in cols]
        total = [jnp.zeros((B, LANES), F32) for c in cols]
        for a in range(B):
            word, weight = own[i, a : a + 1], own[i, B + a : B + a + 1]
            for j in range(J):
                total[j] += jnp.where(words_of[j] == word, weight, F32(0.0))
        for j, c in enumerate(cols):
            values = got[2 * B : 3 * B, c] + got[3 * B : 4 * B, c]
            part_out[d, j : j + 1] = jnp.sum(total[j] * values, axis=0, keepdims=True)
            norms = got[4 * B : 4 * B + 1, c] + got[4 * B + 1 : 4 * B + 2, c]
            part_out[d, J + j : J + j + 1] = norms
        part_out[d, 2 * J : 2 * J + 1] = own[i, 2 * B : 2 * B + 1]

    def far_sends():
        def each(k):
            @pl.when(k >= me_w)
            def _():
                pl.semaphore_wait(go.at[k + 1], S)
                send_word(k)

        loop(W - 1, 4, each)

    def after(i):
        d = order(i)
        if isinstance(i, int) and i == 0:
            pl.when(me_s < S - 1)(lambda: pl.semaphore_wait(go.at[me_w], S - 1 - me_s))
            send_near(True)
            pl.when(late)(far_sends)
        high = me_w + 1 + i < W
        wait_high = jnp.logical_and(early, high)
        mate = jnp.logical_and(below, i == 0)
        pl.when(wait_high)(lambda: pl.semaphore_wait(go.at[me_w + 1 + i], jnp.where(mate, half, S)))
        part_copy(d).start()
        full = jnp.logical_and(wait_high, jnp.logical_not(mate))
        pl.when(jnp.logical_and(full, left))(lambda: send_word(d, half, S))
        pl.when(wait_high)(lambda: send_word(d, 0, half))
        pl.when(jnp.logical_and(full, jnp.logical_not(left)))(lambda: send_word(d, half, S))
        rest_low = jnp.logical_and(jnp.logical_and(early, jnp.logical_not(high)), d > 0)
        pl.when(rest_low)(lambda: send_word(d))
        if isinstance(i, int) and i == 0:
            pl.when(jnp.logical_and(late, me_w > 2))(lambda: send_word(me_w - 1))
        else:
            held_back = jnp.logical_or(i < me_w - 1, jnp.logical_and(i == 1, me_w == 2))
            pl.when(jnp.logical_and(late, held_back))(lambda: send_word(i))

    loop(W, 4, owned)
    if W <= 4:
        gather(0)
        for i in range(W):
            target(i)
            if i + 1 < W:
                gather(i + 1)
                after(i)
    else:
        def step(i):
            gather(i)
            target(i)

        step(0)
        after(0)
        lax.fori_loop(1, W - 1, lambda i, carry: (step(i), after(i), carry)[2], 0)
        step(W - 1)

    pairs = near_ref.shape[0]
    group = 8

    order_of = [turn(i) for i in range(W)] if gram else None

    def lowest_two(base, inner):
        tops = []
        for t in range(2):
            low = second = None
            for v in range(t, width // 8, 2):
                x = base[v * 8 : v * 8 + 8] + inner[v * 8 : v * 8 + 8]
                if low is None:
                    low = x
                elif second is None:
                    low, second = jnp.minimum(low, x), jnp.maximum(low, x)
                else:
                    second = jnp.minimum(second, jnp.maximum(low, x))
                    low = jnp.minimum(low, x)
            tops.append((low, second))
        (l0, s0), (l1, s1) = tops
        return jnp.minimum(l0, l1), jnp.minimum(jnp.maximum(l0, l1), jnp.minimum(s0, s1))

    def block(j, b):
        inner = dot(rt[b], qs[j])
        base = sqb[b]
        for c in range(C):
            a = j * C + c
            if a != b:
                cell = (order_of[j] * C + c) * H + order_of[b // C] * C + b % C
                low_t[cell], next_t[cell] = lowest_two(base, inner[:, c * width : (c + 1) * width])

    def arrive(i):
        w = order_of[i] if gram else turn(i)

        def arrived(slices):
            pltpu.make_async_remote_copy(
                src_ref=held.at[w, pl.ds(0, slices)], dst_ref=held.at[w, pl.ds(0, slices)],
                send_sem=dsend, recv_sem=drecv.at[w],
                device_id=(me_g, me_w, me_s), device_id_type=MESH,
            ).wait_recv()

        if isinstance(i, int):
            arrived(S if i > 0 else S - 1)
        else:
            pl.when(i > 0)(lambda: arrived(S))
            pl.when(i == 0)(lambda: arrived(S - 1))
        for c in range(C):
            h = i * C + c if gram else w * C + c
            full = jnp.concatenate([held[w, s, c] for s in range(S)], axis=0)
            if gram:
                qs[i, :, c * width : (c + 1) * width] = full
            else:
                qs[h] = full
            wide = full.astype(F32)
            turned = jnp.transpose(wide)
            rt[h] = (turned * -2.0).astype(BF16)
            count = cnt_ref[w * stored + from_ref[w, c, me_s]]
            down = lax.broadcasted_iota(I32, (width, width), 0)
            square = jnp.sum(turned * turned, axis=1, keepdims=True)
            sqb[h] = jnp.where(down < count, square, F32(1e30))
            flat = jnp.sum(wide * wide, axis=0, keepdims=True)
            live = jnp.where(lax.broadcasted_iota(I32, (8, width), 1) < count, F32(1.0), F32(0.0))
            info[w * C + c] = jnp.where(lax.broadcasted_iota(I32, (8, width), 0) == 0, flat, live)
        if gram:
            for b in range((i + 1) * C):
                block(i, b)
            for j in range(i):
                for c in range(C):
                    block(j, i * C + c)

    def whole(ref, send_sem, recv_sem):
        return pltpu.make_async_remote_copy(
            src_ref=ref, dst_ref=ref, send_sem=send_sem, recv_sem=recv_sem,
            device_id=(me_g, me_w, me_s), device_id_type=MESH,
        )

    def similarity():
        whole(part_in.at[pl.ds(0, W - 1)], psend, precv).wait_recv()
        total = part_out[W - 1]
        for d in range(W - 1):
            total += part_in[d]
        cosine = total[0:J] / jnp.sqrt(total[2 * J : 2 * J + 1] * total[J : 2 * J])
        spread = lax.broadcasted_iota(I32, (R, LANES), 1) % R == lax.broadcasted_iota(I32, (R, LANES), 0)
        out_cols = ceil_to(K, LANES)
        deep = lax.broadcasted_iota(I32, (LANES, out_cols), 0) // R
        across = lax.broadcasted_iota(I32, (LANES, out_cols), 1)
        result = jnp.zeros((R, out_cols), F32)
        for j in range(J):
            place = jnp.where(across == deep + j * KK, F32(1.0), F32(0.0)).astype(BF16)
            for piece in pieces(jnp.where(spread, cosine[j : j + 1], F32(0.0))):
                result += dot(piece, place)
        sim_ref[...] = result[:, 0:K]

    if 2 < W <= 4:
        loop(W - 1, 4, arrive)
        pl.when(me_w >= 0)(similarity)
    else:
        loop(W - 1, 4, arrive)
        similarity()
    arrive(W - 1)

    def match(i):
        for k in range(group):
            p = i * group + k
            a, b = slot_ref[0, p], slot_ref[1, p]
            at = pl.ds(p * 8, 8)
            if gram:
                low_s[at], next_s[at] = low_t[a * H + b], next_t[a * H + b]
            else:
                low_s[at], next_s[at] = lowest_two(sqb[b], dot(rt[b], qs[a]))
            info_s[at] = info[a]

    loop(pairs // group, 4, match)

    rows = [pl.ds(i, pairs, stride=8) for i in range(8)]
    low, second = low_s[rows[0]], next_s[rows[0]]
    for at in rows[1:]:
        l1, s1 = low_s[at], next_s[at]
        second = jnp.minimum(jnp.maximum(low, l1), jnp.minimum(second, s1))
        low = jnp.minimum(low, l1)
    live = info_s[rows[1]] > 0.0
    features = F32(feats * S)
    near_ref[...] = jnp.where(live, (low + info_s[rows[0]]) / features, F32(0.0))
    marg_ref[...] = jnp.where(live, (second - low) / features, F32(0.0))

    whole(outd.at[pl.ds(0, n - 1)], dsend, drecv.at[0]).wait_send()
    whole(part_out.at[pl.ds(0, W - 1)], psend, precv).wait_send()


def finish(*refs):
    sems = refs[6]
    copies = [pltpu.make_async_copy(refs[i], refs[3 + i], sems.at[i]) for i in range(3)]
    for copy in copies:
        copy.start()
    for copy in copies:
        copy.wait()


def local(W, S, word_ids, word_weights, neighbours, descriptors, keypoint_count, send_table, pair_slots):
    B, I = word_ids.shape[1:]
    K = neighbours.shape[0]
    R = I // (W * S)
    KK = LANES // R
    J = -(-K // KK)
    C = send_table.shape[-1]
    TR = ceil_to(4 * B + 2, 16)
    KP = ceil_to(J * KK, 16)
    NP = ceil_to(2 * J + 1, 8)
    H = W * C
    stored, feats, width = descriptors.shape
    pairs = pair_slots.shape[2]
    gram = W <= 4 and C > 1 and H * H <= 2 * pairs
    vmem = pl.BlockSpec(memory_space=pltpu.VMEM)
    results = ((R, K), (pairs, width), (pairs, width))
    parts = pl.pallas_call(
        functools.partial(kernel, W, S, (B, I, K, R, KK, J, C, TR, KP, NP, H)),
        out_shape=tuple(pltpu.VMEM(shape, F32) for shape in results),
        in_specs=[pl.BlockSpec(memory_space=pltpu.HBM)] * 7,
        out_specs=(vmem, vmem, vmem),
        scratch_shapes=[
            pltpu.VMEM((B, I), I32),
            pltpu.VMEM((B, I), F32),
            pltpu.VMEM((K, I), I32),
            pltpu.VMEM(descriptors.shape, BF16),
            pltpu.SMEM(keypoint_count.shape, I32),
            pltpu.SMEM((W, C, S), I32),
            pltpu.SMEM((W, C, S), I32),
            pltpu.SMEM((2, pairs), I32),
            pltpu.VMEM((W * S, C, feats, width), BF16),
            pltpu.VMEM((W, S, C, feats, width), BF16),
            pltpu.VMEM((TR + 2 * KP, I), BF16),
            pltpu.VMEM((KP, I), I32),
            pltpu.VMEM((W, 2 * B + 8, LANES), F32),
            pltpu.VMEM((W, ceil_to(J, 8), LANES), I32),
            pltpu.VMEM((TR, J * LANES), F32),
            pltpu.VMEM((TR, J * LANES), F32),
            pltpu.VMEM((W, NP, LANES), F32),
            pltpu.VMEM((W, NP, LANES), F32),
            pltpu.VMEM((W, width, C * width) if gram else (H, width, width), BF16),
            pltpu.VMEM((H, width, width), BF16),
            pltpu.VMEM((H, width, width), F32),
            pltpu.VMEM((H, 8, width), F32),
            pltpu.VMEM((H * H if gram else 1, 8, width), F32),
            pltpu.VMEM((H * H if gram else 1, 8, width), F32),
            pltpu.VMEM((pairs * 8, width), F32),
            pltpu.VMEM((pairs * 8, width), F32),
            pltpu.VMEM((pairs * 8, width), F32),
            pltpu.SemaphoreType.DMA,
            pltpu.SemaphoreType.DMA((W,)),
            pltpu.SemaphoreType.DMA,
            pltpu.SemaphoreType.DMA,
            pltpu.SemaphoreType.DMA((2,)),
            pltpu.SemaphoreType.REGULAR((W,)),
        ],
        compiler_params=pltpu.CompilerParams(
            collective_id=0, has_side_effects=True, vmem_limit_bytes=LIMIT
        ),
    )(*(pltpu.with_memory_space_constraint(operand, pltpu.HBM) for operand in (
        word_ids[0], word_weights[0], neighbours, descriptors,
        keypoint_count, jnp.swapaxes(send_table, 2, 3), jnp.swapaxes(pair_slots, 2, 3)[0, 0],
    )))
    similarity, nearest, margin = pl.pallas_call(
        finish,
        out_shape=tuple(jax.ShapeDtypeStruct(shape, F32) for shape in results),
        in_specs=[pl.BlockSpec(memory_space=pl.ANY)] * 3,
        out_specs=(pl.BlockSpec(memory_space=pltpu.HBM),) * 3,
        scratch_shapes=[pltpu.SemaphoreType.DMA((3,))],
        compiler_params=pltpu.CompilerParams(vmem_limit_bytes=LIMIT),
    )(*parts)
    return similarity, nearest[None, None], margin[None, None]


def solution(mesh):
    in_specs = (
        P("word", None, "groups"),
        P("word", None, "groups"),
        P(None, "groups"),
        P(("groups", "word"), "sub", None),
        P("groups"),
        P("groups", None, None, None),
        P(("groups", "word"), "sub", None, None),
    )
    out_specs = (
        P(("groups", "word", "sub"), None),
        P(("groups", "word"), "sub", None, None),
        P(("groups", "word"), "sub", None, None),
    )
    body = functools.partial(local, mesh.shape["word"], mesh.shape["sub"])
    return jax.shard_map(body, mesh=mesh, in_specs=in_specs, out_specs=out_specs, check_vma=False)
```

```python
import functools

import jax
import jax.numpy as jnp
from jax import lax
from jax.experimental import pallas as pl
from jax.experimental.pallas import tpu as pltpu
from jax.sharding import PartitionSpec as P

MESH = pl.DeviceIdType.MESH
LANES = 128
LIMIT = 40 * 1024 * 1024
F32, BF16, I32 = jnp.float32, jnp.bfloat16, jnp.int32


def ceil_to(value, step):
    return (value + step - 1) // step * step


def loop(count, limit, body):
    if count <= limit:
        for i in range(count):
            body(i)
    else:
        lax.fori_loop(0, count, lambda i, carry: (body(i), carry)[1], 0)


def pieces(x):
    first = x.astype(BF16)
    return first, (x - first.astype(F32)).astype(BF16)


def dot(a, b):
    return lax.dot_general(a, b, (((1,), (0,)), ((), ())), preferred_element_type=F32)


def onehot(want, rows):
    numbers = lax.broadcasted_iota(I32, (rows, want.shape[-1]), 0)
    return jnp.where(numbers == want, F32(1.0), F32(0.0)).astype(BF16)


def kernel(
    W, S, dims,
    ids_hbm, wts_hbm, nb_hbm, desc_hbm, cnt_hbm, tab_hbm, slot_hbm,
    sim_ref, near_ref, marg_ref,
    ids_ref, wts_ref, nb_ref, desc_ref, cnt_ref, to_ref, from_ref, slot_ref,
    outd, held, table, nbf, own, wanted, got_0, got_1, part_out, part_in,
    qs, rt, sqb, info, low_t, next_t, low_s, next_s, info_s,
    dsend, drecv, psend, precv, go,
):
    B, I, K, R, KK, J, C, TR, KP, NP, H = dims
    gots = got_0, got_1
    gram = qs.shape[0] == W
    me_g, me_w, me_s = lax.axis_index("groups"), lax.axis_index("word"), lax.axis_index("sub")
    n = W * S
    stored, feats, width = desc_ref.shape

    def turn(step):
        if isinstance(step, int) and step == 0:
            return me_w
        inner = early
        place = jnp.where(inner, W - me_w, me_w + W - W // 2) % W
        k = step - 1 + jnp.where(step > place, 1, 0)
        w = jnp.where(inner, W - k, W // 2 + k) % W
        return w if isinstance(step, int) else jnp.where(step == 0, me_w, w)

    def word_at(k):
        return k + jnp.where(me_w <= k, 1, 0)

    def sub_at(j):
        if S & (S - 1):
            return (me_s + j) % S
        sub, bit = me_s, 1
        while bit < S:
            sub += (S - 1 - j) // bit % 2 * (1 - me_s // bit % 2 * 2) * bit
            bit *= 2
        return sub

    def load(sem, source, target):
        return pltpu.make_async_copy(source, target, sem)

    first = [
        load(dsend, tab_hbm.at[me_w], to_ref),
        load(dsend, desc_hbm, desc_ref),
    ]
    rest = [
        load(psend, ids_hbm, ids_ref),
        load(psend, wts_hbm, wts_ref),
        load(psend, nb_hbm, nb_ref),
        load(psend, tab_hbm.at[:, me_w], from_ref),
        load(psend, cnt_hbm, cnt_ref),
        load(psend, slot_hbm, slot_ref),
    ]
    for copy in first:
        copy.start()

    def words(above, body):
        for_each = lambda k: pl.when((k >= me_w) if above else (k < me_w))(lambda: body(word_at(k)))
        loop(W - 1, 4, for_each)

    def subs(above, body):
        loop(S, 8, lambda s: pl.when((s > me_s) if above else (s < me_s))(lambda: body(s)))

    barrier = pltpu.get_barrier_semaphore()

    def signal(sem, w, s):
        pl.semaphore_signal(sem, inc=1, device_id=(me_g, w, s), device_id_type=MESH)

    half, mid = S // 2, W // 2
    paired = W > 1 and S > 1 and not W & (W - 1) and not S & (S - 1)
    below, above = jnp.logical_and(paired, me_w == mid - 1), jnp.logical_and(paired, me_w == mid)
    side = me_s // max(half, 1) * half

    subs(True, lambda s: signal(barrier, me_w, s))
    if paired:
        pl.when(above)(lambda: loop(half, 8, lambda j: signal(barrier, mid - 1, side + j)))
    words(True, lambda w: loop(S, 8, lambda s: signal(barrier, w, s)))
    for copy in rest:
        copy.start()
    lower = me_w * S + me_s + jnp.where(below, half, 0)
    pl.when(lower > 0)(lambda: pl.semaphore_wait(barrier, lower))
    def answer(w):
        mate = jnp.logical_and(above, w == mid - 1)
        if paired:
            pl.when(mate)(lambda: loop(half, 8, lambda j: signal(go.at[me_w], w, half - side + j)))
        pl.when(jnp.logical_not(mate))(lambda: loop(S, 8, lambda s: signal(go.at[me_w], w, s)))

    words(False, answer)
    subs(False, lambda s: signal(go.at[me_w], me_w, s))
    for copy in first:
        copy.wait()

    def pick(slot, w, s):
        for c in range(C):
            outd[slot, c] = desc_ref[to_ref[w, c, s]]

    loop(W - 1, 4, lambda k: loop(S, 8, lambda j: pick(k * S + j, word_at(k), sub_at(j))))
    loop(S, 8, lambda j: pick((W - 1) * S + j, me_w, sub_at(j)))
    for c in range(C):
        held[me_w, me_s, c] = desc_ref[to_ref[me_w, c, me_s]]

    def send(slot, w, s):
        pltpu.make_async_remote_copy(
            src_ref=outd.at[slot], dst_ref=held.at[me_w, me_s],
            send_sem=dsend, recv_sem=drecv.at[me_w],
            device_id=(me_g, w, s), device_id_type=MESH,
        ).start()

    def send_word(k, first=0, last=S):
        loop(last - first, 8, lambda j: send(k * S + first + j, word_at(k), sub_at(first + j)))

    def send_near(above):
        def each(j):
            s = sub_at(j)
            pl.when((s > me_s) if above else (s < me_s))(lambda: send((W - 1) * S + j, me_w, s))

        loop(S, 8, each)

    early = 2 * me_w < W - 1
    late = jnp.logical_not(early)
    left = me_s < half
    if paired:
        pl.when(below)(lambda: send_word(mid - 1, half, S))
    pl.when(jnp.logical_and(me_w > 0, left))(lambda: send_word(0, half, S))
    pl.when(me_w > 0)(lambda: send_word(0, 0, half))
    pl.when(jnp.logical_and(me_w > 0, jnp.logical_not(left)))(lambda: send_word(0, half, S))
    send_near(False)

    for copy in rest:
        copy.wait()

    ids = ids_ref[...]
    table[0:B] = (ids >> 8).astype(F32).astype(BF16)
    table[B : 2 * B] = (ids & 255).astype(F32).astype(BF16)
    for i, piece in enumerate(pieces(wts_ref[...])):
        table[(2 + i) * B : (3 + i) * B] = piece
    nbf[...] = jnp.zeros_like(nbf)
    nbf[0:K] = nb_ref[...]
    near_ids = nbf[...]
    table[TR : TR + KP] = (near_ids >> 8).astype(F32).astype(BF16)
    table[TR + KP : TR + 2 * KP] = (near_ids & 255).astype(F32).astype(BF16)

    chunk = min(I, 256)

    def self_norm(i):
        at = pl.ds(i * chunk if isinstance(i, int) else pl.multiple_of(i * chunk, chunk), chunk)
        here = ids_ref[:, at]
        total = jnp.zeros((B, chunk), F32)
        for a in range(B):
            total += jnp.where(here == ids_ref[a : a + 1, at], wts_ref[a : a + 1, at], F32(0.0))
        norm = jnp.sum(total * wts_ref[:, at], axis=0, keepdims=True)
        row = lax.broadcasted_iota(I32, (16, chunk), 0)
        block = jnp.zeros((16, chunk), F32)
        for k, piece in enumerate(pieces(norm)):
            block = jnp.where(row == k, piece.astype(F32), block)
        table[4 * B : TR, at] = block.astype(BF16)

    loop(I // chunk, 1, self_norm)

    def part_copy(d):
        w = word_at(d)
        return pltpu.make_async_remote_copy(
            src_ref=part_out.at[d], dst_ref=part_in.at[me_w - jnp.where(me_w > w, 1, 0)],
            send_sem=psend, recv_sem=precv,
            device_id=(me_g, w, me_s), device_id_type=MESH,
        )

    lane = lax.broadcasted_iota(I32, (1, LANES), 1)
    digit = lax.broadcasted_iota(I32, (KK, LANES), 0) == lax.broadcasted_iota(I32, (KK, LANES), 1) // R

    def order(i):
        d = (i + jnp.where(early, me_w, 0)) % max(W - 1, 1)
        if isinstance(i, int):
            return d if i < W - 1 else W - 1
        return jnp.where(i < W - 1, d, W - 1)

    def owned(i):
        d = order(i)
        w = jnp.where(d == W - 1, me_w, word_at(d))
        mine = dot(table[...], onehot((w * S + me_s) * R + lane % R, I))
        own[i, 0:B] = mine[0:B] * 256.0 + mine[B : 2 * B]
        own[i, B : 2 * B] = mine[2 * B : 3 * B] + mine[3 * B : 4 * B]
        own[i, 2 * B : 2 * B + 1] = mine[4 * B : 4 * B + 1] + mine[4 * B + 1 : 4 * B + 2]
        listed = mine[TR : TR + KP] * 256.0 + mine[TR + KP : TR + 2 * KP]
        for j in range(J):
            chosen = jnp.where(digit, listed[j * KK : (j + 1) * KK], F32(0.0))
            wanted[i, j : j + 1] = jnp.sum(chosen, axis=0, keepdims=True).astype(I32)

    def gather(i):
        got = gots[i % 2] if isinstance(i, int) else gots[0]
        for j in range(J):
            got[:, j * LANES : (j + 1) * LANES] = dot(table[0:TR], onehot(wanted[i, j : j + 1], I))

    def target(i):
        d = order(i)
        got = gots[i % 2] if isinstance(i, int) else gots[0]
        cols = [slice(j * LANES, (j + 1) * LANES) for j in range(J)]
        words_of = [got[0:B, c] * 256.0 + got[B : 2 * B, c] for c in cols]
        total = [jnp.zeros((B, LANES), F32) for c in cols]
        for a in range(B):
            word, weight = own[i, a : a + 1], own[i, B + a : B + a + 1]
            for j in range(J):
                total[j] += jnp.where(words_of[j] == word, weight, F32(0.0))
        for j, c in enumerate(cols):
            values = got[2 * B : 3 * B, c] + got[3 * B : 4 * B, c]
            part_out[d, j : j + 1] = jnp.sum(total[j] * values, axis=0, keepdims=True)
            norms = got[4 * B : 4 * B + 1, c] + got[4 * B + 1 : 4 * B + 2, c]
            part_out[d, J + j : J + j + 1] = norms
        part_out[d, 2 * J : 2 * J + 1] = own[i, 2 * B : 2 * B + 1]

    def far_sends():
        def each(k):
            @pl.when(k >= me_w)
            def _():
                pl.semaphore_wait(go.at[k + 1], S)
                send_word(k)

        loop(W - 1, 4, each)

    def after(i):
        d = order(i)
        if isinstance(i, int) and i == 0:
            pl.when(me_s < S - 1)(lambda: pl.semaphore_wait(go.at[me_w], S - 1 - me_s))
            send_near(True)
            pl.when(late)(far_sends)
        high = me_w + 1 + i < W
        wait_high = jnp.logical_and(early, high)
        mate = jnp.logical_and(below, i == 0)
        pl.when(wait_high)(lambda: pl.semaphore_wait(go.at[me_w + 1 + i], jnp.where(mate, half, S)))
        part_copy(d).start()
        full = jnp.logical_and(wait_high, jnp.logical_not(mate))
        pl.when(jnp.logical_and(full, left))(lambda: send_word(d, half, S))
        pl.when(wait_high)(lambda: send_word(d, 0, half))
        pl.when(jnp.logical_and(full, jnp.logical_not(left)))(lambda: send_word(d, half, S))
        rest_low = jnp.logical_and(jnp.logical_and(early, jnp.logical_not(high)), d > 0)
        pl.when(rest_low)(lambda: send_word(d))
        if isinstance(i, int) and i == 0:
            pl.when(jnp.logical_and(late, me_w > 2))(lambda: send_word(me_w - 1))
        else:
            held_back = jnp.logical_or(i < me_w - 1, jnp.logical_and(i == 1, me_w == 2))
            pl.when(jnp.logical_and(late, held_back))(lambda: send_word(i))

    loop(W, 4, owned)
    if W <= 4:
        gather(0)
        for i in range(W):
            target(i)
            if i + 1 < W:
                gather(i + 1)
                after(i)
    else:
        def step(i):
            gather(i)
            target(i)

        step(0)
        after(0)
        lax.fori_loop(1, W - 1, lambda i, carry: (step(i), after(i), carry)[2], 0)
        step(W - 1)

    pairs = near_ref.shape[0]
    group = 8

    order_of = [turn(i) for i in range(W)] if gram else None

    def lowest_two(base, inner):
        tops = []
        for t in range(2):
            low = second = None
            for v in range(t, width // 8, 2):
                x = base[v * 8 : v * 8 + 8] + inner[v * 8 : v * 8 + 8]
                if low is None:
                    low = x
                elif second is None:
                    low, second = jnp.minimum(low, x), jnp.maximum(low, x)
                else:
                    second = jnp.minimum(second, jnp.maximum(low, x))
                    low = jnp.minimum(low, x)
            tops.append((low, second))
        (l0, s0), (l1, s1) = tops
        return jnp.minimum(l0, l1), jnp.minimum(jnp.maximum(l0, l1), jnp.minimum(s0, s1))

    def block(j, b):
        inner = dot(rt[b], qs[j])
        base = sqb[b]
        for c in range(C):
            a = j * C + c
            if a != b:
                cell = (order_of[j] * C + c) * H + order_of[b // C] * C + b % C
                low_t[cell], next_t[cell] = lowest_two(base, inner[:, c * width : (c + 1) * width])

    def arrive(i):
        w = order_of[i] if gram else turn(i)

        def arrived(slices):
            pltpu.make_async_remote_copy(
                src_ref=held.at[w, pl.ds(0, slices)], dst_ref=held.at[w, pl.ds(0, slices)],
                send_sem=dsend, recv_sem=drecv.at[w],
                device_id=(me_g, me_w, me_s), device_id_type=MESH,
            ).wait_recv()

        if isinstance(i, int):
            arrived(S if i > 0 else S - 1)
        else:
            pl.when(i > 0)(lambda: arrived(S))
            pl.when(i == 0)(lambda: arrived(S - 1))
        for c in range(C):
            h = i * C + c if gram else w * C + c
            full = jnp.concatenate([held[w, s, c] for s in range(S)], axis=0)
            if gram:
                qs[i, :, c * width : (c + 1) * width] = full
            else:
                qs[h] = full
            wide = full.astype(F32)
            turned = jnp.transpose(wide)
            rt[h] = (turned * -2.0).astype(BF16)
            count = cnt_ref[w * stored + from_ref[w, c, me_s]]
            down = lax.broadcasted_iota(I32, (width, width), 0)
            square = jnp.sum(turned * turned, axis=1, keepdims=True)
            sqb[h] = jnp.where(down < count, square, F32(1e30))
            flat = jnp.sum(wide * wide, axis=0, keepdims=True)
            live = jnp.where(lax.broadcasted_iota(I32, (8, width), 1) < count, F32(1.0), F32(0.0))
            info[w * C + c] = jnp.where(lax.broadcasted_iota(I32, (8, width), 0) == 0, flat, live)
        if gram:
            for b in range((i + 1) * C):
                block(i, b)
            for j in range(i):
                for c in range(C):
                    block(j, i * C + c)

    def whole(ref, send_sem, recv_sem):
        return pltpu.make_async_remote_copy(
            src_ref=ref, dst_ref=ref, send_sem=send_sem, recv_sem=recv_sem,
            device_id=(me_g, me_w, me_s), device_id_type=MESH,
        )

    def similarity():
        whole(part_in.at[pl.ds(0, W - 1)], psend, precv).wait_recv()
        total = part_out[W - 1]
        for d in range(W - 1):
            total += part_in[d]
        cosine = total[0:J] / jnp.sqrt(total[2 * J : 2 * J + 1] * total[J : 2 * J])
        spread = lax.broadcasted_iota(I32, (R, LANES), 1) % R == lax.broadcasted_iota(I32, (R, LANES), 0)
        out_cols = ceil_to(K, LANES)
        deep = lax.broadcasted_iota(I32, (LANES, out_cols), 0) // R
        across = lax.broadcasted_iota(I32, (LANES, out_cols), 1)
        result = jnp.zeros((R, out_cols), F32)
        for j in range(J):
            place = jnp.where(across == deep + j * KK, F32(1.0), F32(0.0)).astype(BF16)
            for piece in pieces(jnp.where(spread, cosine[j : j + 1], F32(0.0))):
                result += dot(piece, place)
        sim_ref[...] = result[:, 0:K]

    if 2 < W <= 4:
        arrive(0)
        arrive(1)
        pl.when(me_w % 2 == 1)(similarity)
        loop(W - 3, 4, lambda i: arrive(2 + i))
        pl.when(me_w % 2 == 0)(similarity)
        arrive(W - 1)
    else:
        loop(W - 1, 4, arrive)
        similarity()
        arrive(W - 1)

    def match(i):
        for k in range(group):
            p = i * group + k
            a, b = slot_ref[0, p], slot_ref[1, p]
            at = pl.ds(p * 8, 8)
            if gram:
                low_s[at], next_s[at] = low_t[a * H + b], next_t[a * H + b]
            else:
                low_s[at], next_s[at] = lowest_two(sqb[b], dot(rt[b], qs[a]))
            info_s[at] = info[a]

    loop(pairs // group, 4, match)

    rows = [pl.ds(i, pairs, stride=8) for i in range(8)]
    low, second = low_s[rows[0]], next_s[rows[0]]
    for at in rows[1:]:
        l1, s1 = low_s[at], next_s[at]
        second = jnp.minimum(jnp.maximum(low, l1), jnp.minimum(second, s1))
        low = jnp.minimum(low, l1)
    live = info_s[rows[1]] > 0.0
    features = F32(feats * S)
    near_ref[...] = jnp.where(live, (low + info_s[rows[0]]) / features, F32(0.0))
    marg_ref[...] = jnp.where(live, (second - low) / features, F32(0.0))

    whole(outd.at[pl.ds(0, n - 1)], dsend, drecv.at[0]).wait_send()
    whole(part_out.at[pl.ds(0, W - 1)], psend, precv).wait_send()


def finish(*refs):
    sems = refs[6]
    copies = [pltpu.make_async_copy(refs[i], refs[3 + i], sems.at[i]) for i in range(3)]
    for copy in copies:
        copy.start()
    for copy in copies:
        copy.wait()


def local(W, S, word_ids, word_weights, neighbours, descriptors, keypoint_count, send_table, pair_slots):
    B, I = word_ids.shape[1:]
    K = neighbours.shape[0]
    R = I // (W * S)
    KK = LANES // R
    J = -(-K // KK)
    C = send_table.shape[-1]
    TR = ceil_to(4 * B + 2, 16)
    KP = ceil_to(J * KK, 16)
    NP = ceil_to(2 * J + 1, 8)
    H = W * C
    stored, feats, width = descriptors.shape
    pairs = pair_slots.shape[2]
    gram = W <= 4 and C > 1 and H * H <= 2 * pairs
    vmem = pl.BlockSpec(memory_space=pltpu.VMEM)
    results = ((R, K), (pairs, width), (pairs, width))
    parts = pl.pallas_call(
        functools.partial(kernel, W, S, (B, I, K, R, KK, J, C, TR, KP, NP, H)),
        out_shape=tuple(pltpu.VMEM(shape, F32) for shape in results),
        in_specs=[pl.BlockSpec(memory_space=pltpu.HBM)] * 7,
        out_specs=(vmem, vmem, vmem),
        scratch_shapes=[
            pltpu.VMEM((B, I), I32),
            pltpu.VMEM((B, I), F32),
            pltpu.VMEM((K, I), I32),
            pltpu.VMEM(descriptors.shape, BF16),
            pltpu.SMEM(keypoint_count.shape, I32),
            pltpu.SMEM((W, C, S), I32),
            pltpu.SMEM((W, C, S), I32),
            pltpu.SMEM((2, pairs), I32),
            pltpu.VMEM((W * S, C, feats, width), BF16),
            pltpu.VMEM((W, S, C, feats, width), BF16),
            pltpu.VMEM((TR + 2 * KP, I), BF16),
            pltpu.VMEM((KP, I), I32),
            pltpu.VMEM((W, 2 * B + 8, LANES), F32),
            pltpu.VMEM((W, ceil_to(J, 8), LANES), I32),
            pltpu.VMEM((TR, J * LANES), F32),
            pltpu.VMEM((TR, J * LANES), F32),
            pltpu.VMEM((W, NP, LANES), F32),
            pltpu.VMEM((W, NP, LANES), F32),
            pltpu.VMEM((W, width, C * width) if gram else (H, width, width), BF16),
            pltpu.VMEM((H, width, width), BF16),
            pltpu.VMEM((H, width, width), F32),
            pltpu.VMEM((H, 8, width), F32),
            pltpu.VMEM((H * H if gram else 1, 8, width), F32),
            pltpu.VMEM((H * H if gram else 1, 8, width), F32),
            pltpu.VMEM((pairs * 8, width), F32),
            pltpu.VMEM((pairs * 8, width), F32),
            pltpu.VMEM((pairs * 8, width), F32),
            pltpu.SemaphoreType.DMA,
            pltpu.SemaphoreType.DMA((W,)),
            pltpu.SemaphoreType.DMA,
            pltpu.SemaphoreType.DMA,
            pltpu.SemaphoreType.REGULAR((W,)),
        ],
        compiler_params=pltpu.CompilerParams(
            collective_id=0, has_side_effects=True, vmem_limit_bytes=LIMIT
        ),
    )(*(pltpu.with_memory_space_constraint(operand, pltpu.HBM) for operand in (
        word_ids[0], word_weights[0], neighbours, descriptors,
        keypoint_count, jnp.swapaxes(send_table, 2, 3), jnp.swapaxes(pair_slots, 2, 3)[0, 0],
    )))
    similarity, nearest, margin = pl.pallas_call(
        finish,
        out_shape=tuple(jax.ShapeDtypeStruct(shape, F32) for shape in results),
        in_specs=[pl.BlockSpec(memory_space=pl.ANY)] * 3,
        out_specs=(pl.BlockSpec(memory_space=pltpu.HBM),) * 3,
        scratch_shapes=[pltpu.SemaphoreType.DMA((3,))],
        compiler_params=pltpu.CompilerParams(vmem_limit_bytes=LIMIT),
    )(*parts)
    return similarity, nearest[None, None], margin[None, None]


def solution(mesh):
    in_specs = (
        P("word", None, "groups"),
        P("word", None, "groups"),
        P(None, "groups"),
        P(("groups", "word"), "sub", None),
        P("groups"),
        P("groups", None, None, None),
        P(("groups", "word"), "sub", None, None),
    )
    out_specs = (
        P(("groups", "word", "sub"), None),
        P(("groups", "word"), "sub", None, None),
        P(("groups", "word"), "sub", None, None),
    )
    body = functools.partial(local, mesh.shape["word"], mesh.shape["sub"])
    return jax.shard_map(body, mesh=mesh, in_specs=in_specs, out_specs=out_specs, check_vma=False)
```

```python
import functools

import jax
import jax.numpy as jnp
from jax import lax
from jax.experimental import pallas as pl
from jax.experimental.pallas import tpu as pltpu
from jax.sharding import PartitionSpec as P

MESH = pl.DeviceIdType.MESH
LANES = 128
LIMIT = 40 * 1024 * 1024
F32, BF16, I32 = jnp.float32, jnp.bfloat16, jnp.int32


def ceil_to(value, step):
    return (value + step - 1) // step * step


def loop(count, limit, body):
    if count <= limit:
        for i in range(count):
            body(i)
    else:
        lax.fori_loop(0, count, lambda i, carry: (body(i), carry)[1], 0)


def pieces(x):
    first = x.astype(BF16)
    return first, (x - first.astype(F32)).astype(BF16)


def dot(a, b):
    return lax.dot_general(a, b, (((1,), (0,)), ((), ())), preferred_element_type=F32)


def onehot(want, rows):
    numbers = lax.broadcasted_iota(I32, (rows, want.shape[-1]), 0)
    return jnp.where(numbers == want, F32(1.0), F32(0.0)).astype(BF16)


def kernel(
    W, S, dims,
    ids_hbm, wts_hbm, nb_hbm, desc_hbm, cnt_hbm, tab_hbm, slot_hbm,
    sim_ref, near_ref, marg_ref,
    ids_ref, wts_ref, nb_ref, desc_ref, cnt_ref, to_ref, from_ref, slot_ref,
    outd, held, table, nbf, own, wanted, got_0, got_1, part_out, part_in,
    qs, rt, sqb, info, low_t, next_t, low_s, next_s, info_s,
    dsend, drecv, psend, precv, go,
):
    B, I, K, R, KK, J, C, TR, KP, NP, H = dims
    gots = got_0, got_1
    gram = qs.shape[0] == W
    me_g, me_w, me_s = lax.axis_index("groups"), lax.axis_index("word"), lax.axis_index("sub")
    n = W * S
    stored, feats, width = desc_ref.shape

    def turn(step):
        if isinstance(step, int) and step == 0:
            return me_w
        inner = early
        place = jnp.where(inner, W - me_w, me_w + W - W // 2) % W
        k = step - 1 + jnp.where(step > place, 1, 0)
        w = jnp.where(inner, W - k, W // 2 + k) % W
        return w if isinstance(step, int) else jnp.where(step == 0, me_w, w)

    def word_at(k):
        return k + jnp.where(me_w <= k, 1, 0)

    def sub_at(j):
        if S % 2:
            return (me_s + j) % S
        own_side = me_s // (S // 2) * (S // 2)
        if isinstance(j, int):
            return S // 2 - own_side + j if j < S // 2 else own_side + j - S // 2
        return jnp.where(j < S // 2, S // 2 - own_side + j, own_side + j - S // 2)

    def load(sem, source, target):
        return pltpu.make_async_copy(source, target, sem)

    first = [
        load(dsend, tab_hbm.at[me_w], to_ref),
        load(dsend, desc_hbm, desc_ref),
    ]
    rest = [
        load(psend, ids_hbm, ids_ref),
        load(psend, wts_hbm, wts_ref),
        load(psend, nb_hbm, nb_ref),
        load(psend, tab_hbm.at[:, me_w], from_ref),
        load(psend, cnt_hbm, cnt_ref),
        load(psend, slot_hbm, slot_ref),
    ]
    for copy in first:
        copy.start()

    def words(above, body):
        for_each = lambda k: pl.when((k >= me_w) if above else (k < me_w))(lambda: body(word_at(k)))
        loop(W - 1, 4, for_each)

    def subs(above, body):
        loop(S, 8, lambda s: pl.when((s > me_s) if above else (s < me_s))(lambda: body(s)))

    barrier = pltpu.get_barrier_semaphore()

    def signal(sem, w, s):
        pl.semaphore_signal(sem, inc=1, device_id=(me_g, w, s), device_id_type=MESH)

    half, mid = S // 2, W // 2
    paired = W > 1 and S > 1 and not W & (W - 1) and not S & (S - 1)
    below, above = jnp.logical_and(paired, me_w == mid - 1), jnp.logical_and(paired, me_w == mid)
    side = me_s // max(half, 1) * half

    subs(True, lambda s: signal(barrier, me_w, s))
    if paired:
        pl.when(above)(lambda: loop(half, 8, lambda j: signal(barrier, mid - 1, side + j)))
    words(True, lambda w: loop(S, 8, lambda s: signal(barrier, w, s)))
    for copy in rest:
        copy.start()
    lower = me_w * S + me_s + jnp.where(below, half, 0)
    pl.when(lower > 0)(lambda: pl.semaphore_wait(barrier, lower))
    def answer(w):
        mate = jnp.logical_and(above, w == mid - 1)
        if paired:
            pl.when(mate)(lambda: loop(half, 8, lambda j: signal(go.at[me_w], w, half - side + j)))
        pl.when(jnp.logical_not(mate))(lambda: loop(S, 8, lambda s: signal(go.at[me_w], w, s)))

    words(False, answer)
    subs(False, lambda s: signal(go.at[me_w], me_w, s))
    for copy in first:
        copy.wait()

    def pick(slot, w, s):
        for c in range(C):
            outd[slot, c] = desc_ref[to_ref[w, c, s]]

    loop(W - 1, 4, lambda k: loop(S, 8, lambda j: pick(k * S + j, word_at(k), sub_at(j))))
    loop(S, 8, lambda j: pick((W - 1) * S + j, me_w, sub_at(j)))
    for c in range(C):
        held[me_w, me_s, c] = desc_ref[to_ref[me_w, c, me_s]]

    def send(slot, w, s):
        pltpu.make_async_remote_copy(
            src_ref=outd.at[slot], dst_ref=held.at[me_w, me_s],
            send_sem=dsend, recv_sem=drecv.at[me_w],
            device_id=(me_g, w, s), device_id_type=MESH,
        ).start()

    def send_word(k, first=0, last=S):
        loop(last - first, 8, lambda j: send(k * S + first + j, word_at(k), sub_at(first + j)))

    def send_near(above):
        def each(j):
            s = sub_at(j)
            pl.when((s > me_s) if above else (s < me_s))(lambda: send((W - 1) * S + j, me_w, s))

        loop(S, 8, each)

    early = 2 * me_w < W - 1
    late = jnp.logical_not(early)
    left = me_s < half
    if paired:
        pl.when(below)(lambda: send_word(mid - 1, half, S))
    pl.when(jnp.logical_and(me_w > 0, left))(lambda: send_word(0, half, S))
    pl.when(me_w > 0)(lambda: send_word(0, 0, half))
    pl.when(jnp.logical_and(me_w > 0, jnp.logical_not(left)))(lambda: send_word(0, half, S))
    send_near(False)

    for copy in rest:
        copy.wait()

    ids = ids_ref[...]
    table[0:B] = (ids >> 8).astype(F32).astype(BF16)
    table[B : 2 * B] = (ids & 255).astype(F32).astype(BF16)
    for i, piece in enumerate(pieces(wts_ref[...])):
        table[(2 + i) * B : (3 + i) * B] = piece
    nbf[...] = jnp.zeros_like(nbf)
    nbf[0:K] = nb_ref[...]
    near_ids = nbf[...]
    table[TR : TR + KP] = (near_ids >> 8).astype(F32).astype(BF16)
    table[TR + KP : TR + 2 * KP] = (near_ids & 255).astype(F32).astype(BF16)

    chunk = min(I, 256)

    def self_norm(i):
        at = pl.ds(i * chunk if isinstance(i, int) else pl.multiple_of(i * chunk, chunk), chunk)
        here = ids_ref[:, at]
        total = jnp.zeros((B, chunk), F32)
        for a in range(B):
            total += jnp.where(here == ids_ref[a : a + 1, at], wts_ref[a : a + 1, at], F32(0.0))
        norm = jnp.sum(total * wts_ref[:, at], axis=0, keepdims=True)
        row = lax.broadcasted_iota(I32, (16, chunk), 0)
        block = jnp.zeros((16, chunk), F32)
        for k, piece in enumerate(pieces(norm)):
            block = jnp.where(row == k, piece.astype(F32), block)
        table[4 * B : TR, at] = block.astype(BF16)

    loop(I // chunk, 1, self_norm)

    def part_copy(d):
        w = word_at(d)
        return pltpu.make_async_remote_copy(
            src_ref=part_out.at[d], dst_ref=part_in.at[me_w - jnp.where(me_w > w, 1, 0)],
            send_sem=psend, recv_sem=precv,
            device_id=(me_g, w, me_s), device_id_type=MESH,
        )

    lane = lax.broadcasted_iota(I32, (1, LANES), 1)
    digit = lax.broadcasted_iota(I32, (KK, LANES), 0) == lax.broadcasted_iota(I32, (KK, LANES), 1) // R

    def order(i):
        d = (i + jnp.where(early, me_w, 0)) % max(W - 1, 1)
        if isinstance(i, int):
            return d if i < W - 1 else W - 1
        return jnp.where(i < W - 1, d, W - 1)

    def owned(i):
        d = order(i)
        w = jnp.where(d == W - 1, me_w, word_at(d))
        mine = dot(table[...], onehot((w * S + me_s) * R + lane % R, I))
        own[i, 0:B] = mine[0:B] * 256.0 + mine[B : 2 * B]
        own[i, B : 2 * B] = mine[2 * B : 3 * B] + mine[3 * B : 4 * B]
        own[i, 2 * B : 2 * B + 1] = mine[4 * B : 4 * B + 1] + mine[4 * B + 1 : 4 * B + 2]
        listed = mine[TR : TR + KP] * 256.0 + mine[TR + KP : TR + 2 * KP]
        for j in range(J):
            chosen = jnp.where(digit, listed[j * KK : (j + 1) * KK], F32(0.0))
            wanted[i, j : j + 1] = jnp.sum(chosen, axis=0, keepdims=True).astype(I32)

    def gather(i):
        got = gots[i % 2] if isinstance(i, int) else gots[0]
        for j in range(J):
            got[:, j * LANES : (j + 1) * LANES] = dot(table[0:TR], onehot(wanted[i, j : j + 1], I))

    def target(i):
        d = order(i)
        got = gots[i % 2] if isinstance(i, int) else gots[0]
        cols = [slice(j * LANES, (j + 1) * LANES) for j in range(J)]
        words_of = [got[0:B, c] * 256.0 + got[B : 2 * B, c] for c in cols]
        total = [jnp.zeros((B, LANES), F32) for c in cols]
        for a in range(B):
            word, weight = own[i, a : a + 1], own[i, B + a : B + a + 1]
            for j in range(J):
                total[j] += jnp.where(words_of[j] == word, weight, F32(0.0))
        for j, c in enumerate(cols):
            values = got[2 * B : 3 * B, c] + got[3 * B : 4 * B, c]
            part_out[d, j : j + 1] = jnp.sum(total[j] * values, axis=0, keepdims=True)
            norms = got[4 * B : 4 * B + 1, c] + got[4 * B + 1 : 4 * B + 2, c]
            part_out[d, J + j : J + j + 1] = norms
        part_out[d, 2 * J : 2 * J + 1] = own[i, 2 * B : 2 * B + 1]

    def far_sends():
        def each(k):
            @pl.when(k >= me_w)
            def _():
                pl.semaphore_wait(go.at[k + 1], S)
                send_word(k)

        loop(W - 1, 4, each)

    def after(i):
        d = order(i)
        if isinstance(i, int) and i == 0:
            pl.when(me_s < S - 1)(lambda: pl.semaphore_wait(go.at[me_w], S - 1 - me_s))
            send_near(True)
            pl.when(late)(far_sends)
        high = me_w + 1 + i < W
        wait_high = jnp.logical_and(early, high)
        mate = jnp.logical_and(below, i == 0)
        pl.when(wait_high)(lambda: pl.semaphore_wait(go.at[me_w + 1 + i], jnp.where(mate, half, S)))
        part_copy(d).start()
        full = jnp.logical_and(wait_high, jnp.logical_not(mate))
        pl.when(jnp.logical_and(full, left))(lambda: send_word(d, half, S))
        pl.when(wait_high)(lambda: send_word(d, 0, half))
        pl.when(jnp.logical_and(full, jnp.logical_not(left)))(lambda: send_word(d, half, S))
        rest_low = jnp.logical_and(jnp.logical_and(early, jnp.logical_not(high)), d > 0)
        pl.when(rest_low)(lambda: send_word(d))
        if isinstance(i, int) and i == 0:
            pl.when(jnp.logical_and(late, me_w > 2))(lambda: send_word(me_w - 1))
        else:
            held_back = jnp.logical_or(i < me_w - 1, jnp.logical_and(i == 1, me_w == 2))
            pl.when(jnp.logical_and(late, held_back))(lambda: send_word(i))

    loop(W, 4, owned)
    if W <= 4:
        gather(0)
        for i in range(W):
            target(i)
            if i + 1 < W:
                gather(i + 1)
                after(i)
    else:
        def step(i):
            gather(i)
            target(i)

        step(0)
        after(0)
        lax.fori_loop(1, W - 1, lambda i, carry: (step(i), after(i), carry)[2], 0)
        step(W - 1)

    pairs = near_ref.shape[0]
    group = 8

    order_of = [turn(i) for i in range(W)] if gram else None

    def lowest_two(base, inner):
        tops = []
        for t in range(2):
            low = second = None
            for v in range(t, width // 8, 2):
                x = base[v * 8 : v * 8 + 8] + inner[v * 8 : v * 8 + 8]
                if low is None:
                    low = x
                elif second is None:
                    low, second = jnp.minimum(low, x), jnp.maximum(low, x)
                else:
                    second = jnp.minimum(second, jnp.maximum(low, x))
                    low = jnp.minimum(low, x)
            tops.append((low, second))
        (l0, s0), (l1, s1) = tops
        return jnp.minimum(l0, l1), jnp.minimum(jnp.maximum(l0, l1), jnp.minimum(s0, s1))

    def block(j, b):
        inner = dot(rt[b], qs[j])
        base = sqb[b]
        for c in range(C):
            a = j * C + c
            if a != b:
                cell = (order_of[j] * C + c) * H + order_of[b // C] * C + b % C
                low_t[cell], next_t[cell] = lowest_two(base, inner[:, c * width : (c + 1) * width])

    def arrive(i):
        w = order_of[i] if gram else turn(i)

        def arrived(slices):
            pltpu.make_async_remote_copy(
                src_ref=held.at[w, pl.ds(0, slices)], dst_ref=held.at[w, pl.ds(0, slices)],
                send_sem=dsend, recv_sem=drecv.at[w],
                device_id=(me_g, me_w, me_s), device_id_type=MESH,
            ).wait_recv()

        if isinstance(i, int):
            arrived(S if i > 0 else S - 1)
        else:
            pl.when(i > 0)(lambda: arrived(S))
            pl.when(i == 0)(lambda: arrived(S - 1))
        for c in range(C):
            h = i * C + c if gram else w * C + c
            full = jnp.concatenate([held[w, s, c] for s in range(S)], axis=0)
            if gram:
                qs[i, :, c * width : (c + 1) * width] = full
            else:
                qs[h] = full
            wide = full.astype(F32)
            turned = jnp.transpose(wide)
            rt[h] = (turned * -2.0).astype(BF16)
            count = cnt_ref[w * stored + from_ref[w, c, me_s]]
            down = lax.broadcasted_iota(I32, (width, width), 0)
            square = jnp.sum(turned * turned, axis=1, keepdims=True)
            sqb[h] = jnp.where(down < count, square, F32(1e30))
            flat = jnp.sum(wide * wide, axis=0, keepdims=True)
            live = jnp.where(lax.broadcasted_iota(I32, (8, width), 1) < count, F32(1.0), F32(0.0))
            info[w * C + c] = jnp.where(lax.broadcasted_iota(I32, (8, width), 0) == 0, flat, live)
        if gram:
            for b in range((i + 1) * C):
                block(i, b)
            for j in range(i):
                for c in range(C):
                    block(j, i * C + c)

    def whole(ref, send_sem, recv_sem):
        return pltpu.make_async_remote_copy(
            src_ref=ref, dst_ref=ref, send_sem=send_sem, recv_sem=recv_sem,
            device_id=(me_g, me_w, me_s), device_id_type=MESH,
        )

    def similarity():
        whole(part_in.at[pl.ds(0, W - 1)], psend, precv).wait_recv()
        total = part_out[W - 1]
        for d in range(W - 1):
            total += part_in[d]
        cosine = total[0:J] / jnp.sqrt(total[2 * J : 2 * J + 1] * total[J : 2 * J])
        spread = lax.broadcasted_iota(I32, (R, LANES), 1) % R == lax.broadcasted_iota(I32, (R, LANES), 0)
        out_cols = ceil_to(K, LANES)
        deep = lax.broadcasted_iota(I32, (LANES, out_cols), 0) // R
        across = lax.broadcasted_iota(I32, (LANES, out_cols), 1)
        result = jnp.zeros((R, out_cols), F32)
        for j in range(J):
            place = jnp.where(across == deep + j * KK, F32(1.0), F32(0.0)).astype(BF16)
            for piece in pieces(jnp.where(spread, cosine[j : j + 1], F32(0.0))):
                result += dot(piece, place)
        sim_ref[...] = result[:, 0:K]

    if 2 < W <= 4:
        arrive(0)
        arrive(1)
        pl.when(me_w % 2 == 1)(similarity)
        loop(W - 3, 4, lambda i: arrive(2 + i))
        pl.when(jnp.logical_and(me_w % 2 == 0, me_w > 0))(similarity)
        arrive(W - 1)
        pl.when(me_w == 0)(similarity)
    else:
        loop(W - 1, 4, arrive)
        similarity()
        arrive(W - 1)

    def match(i):
        for k in range(group):
            p = i * group + k
            a, b = slot_ref[0, p], slot_ref[1, p]
            at = pl.ds(p * 8, 8)
            if gram:
                low_s[at], next_s[at] = low_t[a * H + b], next_t[a * H + b]
            else:
                low_s[at], next_s[at] = lowest_two(sqb[b], dot(rt[b], qs[a]))
            info_s[at] = info[a]

    loop(pairs // group, 4, match)

    rows = [pl.ds(i, pairs, stride=8) for i in range(8)]
    low, second = low_s[rows[0]], next_s[rows[0]]
    for at in rows[1:]:
        l1, s1 = low_s[at], next_s[at]
        second = jnp.minimum(jnp.maximum(low, l1), jnp.minimum(second, s1))
        low = jnp.minimum(low, l1)
    live = info_s[rows[1]] > 0.0
    scale = F32(1.0 / (feats * S))
    near_ref[...] = jnp.where(live, (low + info_s[rows[0]]) * scale, F32(0.0))
    marg_ref[...] = jnp.where(live, (second - low) * scale, F32(0.0))

    whole(outd.at[pl.ds(0, n - 1)], dsend, drecv.at[0]).wait_send()
    whole(part_out.at[pl.ds(0, W - 1)], psend, precv).wait_send()


def finish(*refs):
    sems = refs[6]
    copies = [pltpu.make_async_copy(refs[i], refs[3 + i], sems.at[i]) for i in range(3)]
    for copy in copies:
        copy.start()
    for copy in copies:
        copy.wait()


def local(W, S, word_ids, word_weights, neighbours, descriptors, keypoint_count, send_table, pair_slots):
    B, I = word_ids.shape[1:]
    K = neighbours.shape[0]
    R = I // (W * S)
    KK = LANES // R
    J = -(-K // KK)
    C = send_table.shape[-1]
    TR = ceil_to(4 * B + 2, 16)
    KP = ceil_to(J * KK, 16)
    NP = ceil_to(2 * J + 1, 8)
    H = W * C
    stored, feats, width = descriptors.shape
    pairs = pair_slots.shape[2]
    gram = W <= 4 and C > 1 and H * H <= 2 * pairs
    vmem = pl.BlockSpec(memory_space=pltpu.VMEM)
    results = ((R, K), (pairs, width), (pairs, width))
    parts = pl.pallas_call(
        functools.partial(kernel, W, S, (B, I, K, R, KK, J, C, TR, KP, NP, H)),
        out_shape=tuple(pltpu.VMEM(shape, F32) for shape in results),
        in_specs=[pl.BlockSpec(memory_space=pltpu.HBM)] * 7,
        out_specs=(vmem, vmem, vmem),
        scratch_shapes=[
            pltpu.VMEM((B, I), I32),
            pltpu.VMEM((B, I), F32),
            pltpu.VMEM((K, I), I32),
            pltpu.VMEM(descriptors.shape, BF16),
            pltpu.SMEM(keypoint_count.shape, I32),
            pltpu.SMEM((W, C, S), I32),
            pltpu.SMEM((W, C, S), I32),
            pltpu.SMEM((2, pairs), I32),
            pltpu.VMEM((W * S, C, feats, width), BF16),
            pltpu.VMEM((W, S, C, feats, width), BF16),
            pltpu.VMEM((TR + 2 * KP, I), BF16),
            pltpu.VMEM((KP, I), I32),
            pltpu.VMEM((W, 2 * B + 8, LANES), F32),
            pltpu.VMEM((W, ceil_to(J, 8), LANES), I32),
            pltpu.VMEM((TR, J * LANES), F32),
            pltpu.VMEM((TR, J * LANES), F32),
            pltpu.VMEM((W, NP, LANES), F32),
            pltpu.VMEM((W, NP, LANES), F32),
            pltpu.VMEM((W, width, C * width) if gram else (H, width, width), BF16),
            pltpu.VMEM((H, width, width), BF16),
            pltpu.VMEM((H, width, width), F32),
            pltpu.VMEM((H, 8, width), F32),
            pltpu.VMEM((H * H if gram else 1, 8, width), F32),
            pltpu.VMEM((H * H if gram else 1, 8, width), F32),
            pltpu.VMEM((pairs * 8, width), F32),
            pltpu.VMEM((pairs * 8, width), F32),
            pltpu.VMEM((pairs * 8, width), F32),
            pltpu.SemaphoreType.DMA,
            pltpu.SemaphoreType.DMA((W,)),
            pltpu.SemaphoreType.DMA,
            pltpu.SemaphoreType.DMA,
            pltpu.SemaphoreType.REGULAR((W,)),
        ],
        compiler_params=pltpu.CompilerParams(
            collective_id=0, has_side_effects=True, vmem_limit_bytes=LIMIT
        ),
    )(*(pltpu.with_memory_space_constraint(operand, pltpu.HBM) for operand in (
        word_ids[0], word_weights[0], neighbours, descriptors,
        keypoint_count, jnp.swapaxes(send_table, 2, 3), jnp.swapaxes(pair_slots, 2, 3)[0, 0],
    )))
    similarity, nearest, margin = pl.pallas_call(
        finish,
        out_shape=tuple(jax.ShapeDtypeStruct(shape, F32) for shape in results),
        in_specs=[pl.BlockSpec(memory_space=pl.ANY)] * 3,
        out_specs=(pl.BlockSpec(memory_space=pltpu.HBM),) * 3,
        scratch_shapes=[pltpu.SemaphoreType.DMA((3,))],
        compiler_params=pltpu.CompilerParams(vmem_limit_bytes=LIMIT),
    )(*parts)
    return similarity, nearest[None, None], margin[None, None]


def solution(mesh):
    in_specs = (
        P("word", None, "groups"),
        P("word", None, "groups"),
        P(None, "groups"),
        P(("groups", "word"), "sub", None),
        P("groups"),
        P("groups", None, None, None),
        P(("groups", "word"), "sub", None, None),
    )
    out_specs = (
        P(("groups", "word", "sub"), None),
        P(("groups", "word"), "sub", None, None),
        P(("groups", "word"), "sub", None, None),
    )
    body = functools.partial(local, mesh.shape["word"], mesh.shape["sub"])
    return jax.shard_map(body, mesh=mesh, in_specs=in_specs, out_specs=out_specs, check_vma=False)
```

```python
import functools

import jax
import jax.numpy as jnp
from jax import lax
from jax.experimental import pallas as pl
from jax.experimental.pallas import tpu as pltpu
from jax.sharding import PartitionSpec as P

MESH = pl.DeviceIdType.MESH
LANES = 128
LIMIT = 40 * 1024 * 1024
F32, BF16, I32 = jnp.float32, jnp.bfloat16, jnp.int32


def ceil_to(value, step):
    return (value + step - 1) // step * step


def loop(count, limit, body):
    if count <= limit:
        for i in range(count):
            body(i)
    else:
        lax.fori_loop(0, count, lambda i, carry: (body(i), carry)[1], 0)


def pieces(x):
    first = x.astype(BF16)
    return first, (x - first.astype(F32)).astype(BF16)


def dot(a, b):
    return lax.dot_general(a, b, (((1,), (0,)), ((), ())), preferred_element_type=F32)


def onehot(want, rows):
    numbers = lax.broadcasted_iota(I32, (rows, want.shape[-1]), 0)
    return jnp.where(numbers == want, F32(1.0), F32(0.0)).astype(BF16)


def kernel(
    W, S, dims,
    ids_hbm, wts_hbm, nb_hbm, desc_hbm, cnt_hbm, tab_hbm, slot_hbm,
    sim_ref, near_ref, marg_ref,
    ids_ref, wts_ref, nb_ref, desc_ref, cnt_ref, to_ref, from_ref, slot_ref,
    outd, held, table, nbf, own, wanted, got_0, got_1, part_out, part_in,
    qs, rt, sqb, info, low_t, next_t, low_s, next_s, info_s,
    dsend, drecv, psend, precv, go,
):
    B, I, K, R, KK, J, C, TR, KP, NP, H = dims
    gots = got_0, got_1
    gram = qs.shape[0] == W
    me_g, me_w, me_s = lax.axis_index("groups"), lax.axis_index("word"), lax.axis_index("sub")
    n = W * S
    stored, feats, width = desc_ref.shape

    def turn(step):
        if isinstance(step, int) and step == 0:
            return me_w
        inner = early
        place = jnp.where(inner, W - me_w, me_w + W - W // 2) % W
        k = step - 1 + jnp.where(step > place, 1, 0)
        w = jnp.where(inner, W - k, W // 2 + k) % W
        return w if isinstance(step, int) else jnp.where(step == 0, me_w, w)

    def word_at(k):
        return k + jnp.where(me_w <= k, 1, 0)

    def sub_at(j):
        if S % 2:
            return (me_s + j) % S
        own_side = me_s // (S // 2) * (S // 2)
        if isinstance(j, int):
            return S // 2 - own_side + j if j < S // 2 else own_side + j - S // 2
        return jnp.where(j < S // 2, S // 2 - own_side + j, own_side + j - S // 2)

    def load(sem, source, target):
        return pltpu.make_async_copy(source, target, sem)

    first = [
        load(dsend, tab_hbm.at[me_w], to_ref),
        load(dsend, desc_hbm, desc_ref),
    ]
    rest = [
        load(psend, ids_hbm, ids_ref),
        load(psend, wts_hbm, wts_ref),
        load(psend, nb_hbm, nb_ref),
        load(psend, tab_hbm.at[:, me_w], from_ref),
        load(psend, cnt_hbm, cnt_ref),
        load(psend, slot_hbm, slot_ref),
    ]
    for copy in first:
        copy.start()

    def words(above, body):
        for_each = lambda k: pl.when((k >= me_w) if above else (k < me_w))(lambda: body(word_at(k)))
        loop(W - 1, 4, for_each)

    def subs(above, body):
        loop(S, 8, lambda s: pl.when((s > me_s) if above else (s < me_s))(lambda: body(s)))

    barrier = pltpu.get_barrier_semaphore()

    def signal(sem, w, s):
        pl.semaphore_signal(sem, inc=1, device_id=(me_g, w, s), device_id_type=MESH)

    half, mid = S // 2, W // 2
    paired = W > 1 and S > 1 and not W & (W - 1) and not S & (S - 1)
    below, above = jnp.logical_and(paired, me_w == mid - 1), jnp.logical_and(paired, me_w == mid)
    side = me_s // max(half, 1) * half

    subs(True, lambda s: signal(barrier, me_w, s))
    if paired:
        pl.when(above)(lambda: loop(half, 8, lambda j: signal(barrier, mid - 1, side + j)))
    words(True, lambda w: loop(S, 8, lambda s: signal(barrier, w, s)))
    for copy in rest:
        copy.start()
    lower = me_w * S + me_s + jnp.where(below, half, 0)
    pl.when(lower > 0)(lambda: pl.semaphore_wait(barrier, lower))
    def answer(w):
        mate = jnp.logical_and(above, w == mid - 1)
        if paired:
            pl.when(mate)(lambda: loop(half, 8, lambda j: signal(go.at[me_w], w, half - side + j)))
        pl.when(jnp.logical_not(mate))(lambda: loop(S, 8, lambda s: signal(go.at[me_w], w, s)))

    words(False, answer)
    subs(False, lambda s: signal(go.at[me_w], me_w, s))
    for copy in first:
        copy.wait()

    def pick(slot, w, s):
        for c in range(C):
            outd[slot, c] = desc_ref[to_ref[w, c, s]]

    loop(W - 1, 4, lambda k: loop(S, 8, lambda j: pick(k * S + j, word_at(k), sub_at(j))))
    loop(S, 8, lambda j: pick((W - 1) * S + j, me_w, sub_at(j)))
    for c in range(C):
        held[me_w, me_s, c] = desc_ref[to_ref[me_w, c, me_s]]

    def send(slot, w, s):
        pltpu.make_async_remote_copy(
            src_ref=outd.at[slot], dst_ref=held.at[me_w, me_s],
            send_sem=dsend, recv_sem=drecv.at[me_w],
            device_id=(me_g, w, s), device_id_type=MESH,
        ).start()

    def send_word(k, first=0, last=S):
        loop(last - first, 8, lambda j: send(k * S + first + j, word_at(k), sub_at(first + j)))

    def send_near(above):
        def each(j):
            s = sub_at(j)
            pl.when((s > me_s) if above else (s < me_s))(lambda: send((W - 1) * S + j, me_w, s))

        loop(S, 8, each)

    early = 2 * me_w < W - 1
    late = jnp.logical_not(early)
    left = me_s < half
    if paired:
        pl.when(below)(lambda: send_word(mid - 1, half, S))
    pl.when(jnp.logical_and(me_w > 0, left))(lambda: send_word(0, half, S))
    pl.when(me_w > 0)(lambda: send_word(0, 0, half))
    pl.when(jnp.logical_and(me_w > 0, jnp.logical_not(left)))(lambda: send_word(0, half, S))

    for copy in rest:
        copy.wait()

    ids = ids_ref[...]
    table[0:B] = (ids >> 8).astype(F32).astype(BF16)
    table[B : 2 * B] = (ids & 255).astype(F32).astype(BF16)
    for i, piece in enumerate(pieces(wts_ref[...])):
        table[(2 + i) * B : (3 + i) * B] = piece
    nbf[...] = jnp.zeros_like(nbf)
    nbf[0:K] = nb_ref[...]
    near_ids = nbf[...]
    table[TR : TR + KP] = (near_ids >> 8).astype(F32).astype(BF16)
    table[TR + KP : TR + 2 * KP] = (near_ids & 255).astype(F32).astype(BF16)

    chunk = min(I, 256)

    def self_norm(i):
        at = pl.ds(i * chunk if isinstance(i, int) else pl.multiple_of(i * chunk, chunk), chunk)
        here = ids_ref[:, at]
        total = jnp.zeros((B, chunk), F32)
        for a in range(B):
            total += jnp.where(here == ids_ref[a : a + 1, at], wts_ref[a : a + 1, at], F32(0.0))
        norm = jnp.sum(total * wts_ref[:, at], axis=0, keepdims=True)
        row = lax.broadcasted_iota(I32, (16, chunk), 0)
        block = jnp.zeros((16, chunk), F32)
        for k, piece in enumerate(pieces(norm)):
            block = jnp.where(row == k, piece.astype(F32), block)
        table[4 * B : TR, at] = block.astype(BF16)

    loop(I // chunk, 1, self_norm)

    def part_copy(d):
        w = word_at(d)
        return pltpu.make_async_remote_copy(
            src_ref=part_out.at[d], dst_ref=part_in.at[me_w - jnp.where(me_w > w, 1, 0)],
            send_sem=psend, recv_sem=precv,
            device_id=(me_g, w, me_s), device_id_type=MESH,
        )

    lane = lax.broadcasted_iota(I32, (1, LANES), 1)
    digit = lax.broadcasted_iota(I32, (KK, LANES), 0) == lax.broadcasted_iota(I32, (KK, LANES), 1) // R

    def order(i):
        d = (i + jnp.where(early, me_w, 0)) % max(W - 1, 1)
        if isinstance(i, int):
            return d if i < W - 1 else W - 1
        return jnp.where(i < W - 1, d, W - 1)

    def owned(i):
        d = order(i)
        w = jnp.where(d == W - 1, me_w, word_at(d))
        mine = dot(table[...], onehot((w * S + me_s) * R + lane % R, I))
        own[i, 0:B] = mine[0:B] * 256.0 + mine[B : 2 * B]
        own[i, B : 2 * B] = mine[2 * B : 3 * B] + mine[3 * B : 4 * B]
        own[i, 2 * B : 2 * B + 1] = mine[4 * B : 4 * B + 1] + mine[4 * B + 1 : 4 * B + 2]
        listed = mine[TR : TR + KP] * 256.0 + mine[TR + KP : TR + 2 * KP]
        for j in range(J):
            chosen = jnp.where(digit, listed[j * KK : (j + 1) * KK], F32(0.0))
            wanted[i, j : j + 1] = jnp.sum(chosen, axis=0, keepdims=True).astype(I32)

    def gather(i):
        got = gots[i % 2] if isinstance(i, int) else gots[0]
        for j in range(J):
            got[:, j * LANES : (j + 1) * LANES] = dot(table[0:TR], onehot(wanted[i, j : j + 1], I))

    def target(i):
        d = order(i)
        got = gots[i % 2] if isinstance(i, int) else gots[0]
        cols = [slice(j * LANES, (j + 1) * LANES) for j in range(J)]
        words_of = [got[0:B, c] * 256.0 + got[B : 2 * B, c] for c in cols]
        total = [jnp.zeros((B, LANES), F32) for c in cols]
        for a in range(B):
            word, weight = own[i, a : a + 1], own[i, B + a : B + a + 1]
            for j in range(J):
                total[j] += jnp.where(words_of[j] == word, weight, F32(0.0))
        for j, c in enumerate(cols):
            values = got[2 * B : 3 * B, c] + got[3 * B : 4 * B, c]
            part_out[d, j : j + 1] = jnp.sum(total[j] * values, axis=0, keepdims=True)
            norms = got[4 * B : 4 * B + 1, c] + got[4 * B + 1 : 4 * B + 2, c]
            part_out[d, J + j : J + j + 1] = norms
        part_out[d, 2 * J : 2 * J + 1] = own[i, 2 * B : 2 * B + 1]

    def far_sends():
        def each(k):
            @pl.when(k >= me_w)
            def _():
                pl.semaphore_wait(go.at[k + 1], S)
                send_word(k)

        loop(W - 1, 4, each)

    def after(i):
        d = order(i)
        if isinstance(i, int) and i == 0:
            pl.when(me_s < S - 1)(lambda: pl.semaphore_wait(go.at[me_w], S - 1 - me_s))
            pl.when(late)(far_sends)
        high = me_w + 1 + i < W
        wait_high = jnp.logical_and(early, high)
        mate = jnp.logical_and(below, i == 0)
        pl.when(wait_high)(lambda: pl.semaphore_wait(go.at[me_w + 1 + i], jnp.where(mate, half, S)))
        part_copy(d).start()
        full = jnp.logical_and(wait_high, jnp.logical_not(mate))
        pl.when(jnp.logical_and(full, left))(lambda: send_word(d, half, S))
        pl.when(wait_high)(lambda: send_word(d, 0, half))
        pl.when(jnp.logical_and(full, jnp.logical_not(left)))(lambda: send_word(d, half, S))
        if isinstance(i, int) and i == 0:
            send_near(False)
            send_near(True)
        rest_low = jnp.logical_and(jnp.logical_and(early, jnp.logical_not(high)), d > 0)
        pl.when(rest_low)(lambda: send_word(d))
        if isinstance(i, int) and i == 0:
            pl.when(jnp.logical_and(late, me_w > 2))(lambda: send_word(me_w - 1))
        else:
            held_back = jnp.logical_or(i < me_w - 1, jnp.logical_and(i == 1, me_w == 2))
            pl.when(jnp.logical_and(late, held_back))(lambda: send_word(i))

    loop(W, 4, owned)
    if W <= 4:
        gather(0)
        for i in range(W):
            target(i)
            if i + 1 < W:
                gather(i + 1)
                after(i)
    else:
        def step(i):
            gather(i)
            target(i)

        step(0)
        after(0)
        lax.fori_loop(1, W - 1, lambda i, carry: (step(i), after(i), carry)[2], 0)
        step(W - 1)

    pairs = near_ref.shape[0]
    group = 8

    order_of = [turn(i) for i in range(W)] if gram else None

    def lowest_two(base, inner):
        tops = []
        for t in range(2):
            low = second = None
            for v in range(t, width // 8, 2):
                x = base[v * 8 : v * 8 + 8] + inner[v * 8 : v * 8 + 8]
                if low is None:
                    low = x
                elif second is None:
                    low, second = jnp.minimum(low, x), jnp.maximum(low, x)
                else:
                    second = jnp.minimum(second, jnp.maximum(low, x))
                    low = jnp.minimum(low, x)
            tops.append((low, second))
        (l0, s0), (l1, s1) = tops
        return jnp.minimum(l0, l1), jnp.minimum(jnp.maximum(l0, l1), jnp.minimum(s0, s1))

    def block(j, b):
        inner = dot(rt[b], qs[j])
        base = sqb[b]
        for c in range(C):
            a = j * C + c
            if a != b:
                cell = (order_of[j] * C + c) * H + order_of[b // C] * C + b % C
                low_t[cell], next_t[cell] = lowest_two(base, inner[:, c * width : (c + 1) * width])

    def arrive(i):
        w = order_of[i] if gram else turn(i)

        def arrived(slices):
            pltpu.make_async_remote_copy(
                src_ref=held.at[w, pl.ds(0, slices)], dst_ref=held.at[w, pl.ds(0, slices)],
                send_sem=dsend, recv_sem=drecv.at[w],
                device_id=(me_g, me_w, me_s), device_id_type=MESH,
            ).wait_recv()

        if isinstance(i, int):
            arrived(S if i > 0 else S - 1)
        else:
            pl.when(i > 0)(lambda: arrived(S))
            pl.when(i == 0)(lambda: arrived(S - 1))
        for c in range(C):
            h = i * C + c if gram else w * C + c
            full = jnp.concatenate([held[w, s, c] for s in range(S)], axis=0)
            if gram:
                qs[i, :, c * width : (c + 1) * width] = full
            else:
                qs[h] = full
            wide = full.astype(F32)
            turned = jnp.transpose(wide)
            rt[h] = (turned * -2.0).astype(BF16)
            count = cnt_ref[w * stored + from_ref[w, c, me_s]]
            down = lax.broadcasted_iota(I32, (width, width), 0)
            square = jnp.sum(turned * turned, axis=1, keepdims=True)
            sqb[h] = jnp.where(down < count, square, F32(1e30))
            flat = jnp.sum(wide * wide, axis=0, keepdims=True)
            live = jnp.where(lax.broadcasted_iota(I32, (8, width), 1) < count, F32(1.0), F32(0.0))
            info[w * C + c] = jnp.where(lax.broadcasted_iota(I32, (8, width), 0) == 0, flat, live)
        if gram:
            for b in range((i + 1) * C):
                block(i, b)
            for j in range(i):
                for c in range(C):
                    block(j, i * C + c)

    def whole(ref, send_sem, recv_sem):
        return pltpu.make_async_remote_copy(
            src_ref=ref, dst_ref=ref, send_sem=send_sem, recv_sem=recv_sem,
            device_id=(me_g, me_w, me_s), device_id_type=MESH,
        )

    def similarity():
        whole(part_in.at[pl.ds(0, W - 1)], psend, precv).wait_recv()
        total = part_out[W - 1]
        for d in range(W - 1):
            total += part_in[d]
        cosine = total[0:J] / jnp.sqrt(total[2 * J : 2 * J + 1] * total[J : 2 * J])
        spread = lax.broadcasted_iota(I32, (R, LANES), 1) % R == lax.broadcasted_iota(I32, (R, LANES), 0)
        out_cols = ceil_to(K, LANES)
        deep = lax.broadcasted_iota(I32, (LANES, out_cols), 0) // R
        across = lax.broadcasted_iota(I32, (LANES, out_cols), 1)
        result = jnp.zeros((R, out_cols), F32)
        for j in range(J):
            place = jnp.where(across == deep + j * KK, F32(1.0), F32(0.0)).astype(BF16)
            for piece in pieces(jnp.where(spread, cosine[j : j + 1], F32(0.0))):
                result += dot(piece, place)
        sim_ref[...] = result[:, 0:K]

    if 2 < W <= 4:
        arrive(0)
        arrive(1)
        pl.when(me_w % 2 == 1)(similarity)
        loop(W - 3, 4, lambda i: arrive(2 + i))
        pl.when(jnp.logical_and(me_w % 2 == 0, me_w > 0))(similarity)
        arrive(W - 1)
        pl.when(me_w == 0)(similarity)
    else:
        loop(W - 1, 4, arrive)
        similarity()
        arrive(W - 1)

    def match(i):
        for k in range(group):
            p = i * group + k
            a, b = slot_ref[0, p], slot_ref[1, p]
            at = pl.ds(p * 8, 8)
            if gram:
                low_s[at], next_s[at] = low_t[a * H + b], next_t[a * H + b]
            else:
                low_s[at], next_s[at] = lowest_two(sqb[b], dot(rt[b], qs[a]))
            info_s[at] = info[a]

    loop(pairs // group, 4, match)

    rows = [pl.ds(i, pairs, stride=8) for i in range(8)]
    low, second = low_s[rows[0]], next_s[rows[0]]
    for at in rows[1:]:
        l1, s1 = low_s[at], next_s[at]
        second = jnp.minimum(jnp.maximum(low, l1), jnp.minimum(second, s1))
        low = jnp.minimum(low, l1)
    live = info_s[rows[1]] > 0.0
    scale = F32(1.0 / (feats * S))
    near_ref[...] = jnp.where(live, (low + info_s[rows[0]]) * scale, F32(0.0))
    marg_ref[...] = jnp.where(live, (second - low) * scale, F32(0.0))

    whole(outd.at[pl.ds(0, n - 1)], dsend, drecv.at[0]).wait_send()
    whole(part_out.at[pl.ds(0, W - 1)], psend, precv).wait_send()


def finish(*refs):
    sems = refs[6]
    copies = [pltpu.make_async_copy(refs[i], refs[3 + i], sems) for i in range(3)]
    for copy in copies:
        copy.start()
    for copy in copies:
        copy.wait()


def local(W, S, word_ids, word_weights, neighbours, descriptors, keypoint_count, send_table, pair_slots):
    B, I = word_ids.shape[1:]
    K = neighbours.shape[0]
    R = I // (W * S)
    KK = LANES // R
    J = -(-K // KK)
    C = send_table.shape[-1]
    TR = ceil_to(4 * B + 2, 16)
    KP = ceil_to(J * KK, 16)
    NP = ceil_to(2 * J + 1, 8)
    H = W * C
    stored, feats, width = descriptors.shape
    pairs = pair_slots.shape[2]
    gram = W <= 4 and C > 1 and H * H <= 2 * pairs
    vmem = pl.BlockSpec(memory_space=pltpu.VMEM)
    results = ((R, K), (pairs, width), (pairs, width))
    parts = pl.pallas_call(
        functools.partial(kernel, W, S, (B, I, K, R, KK, J, C, TR, KP, NP, H)),
        out_shape=tuple(pltpu.VMEM(shape, F32) for shape in results),
        in_specs=[pl.BlockSpec(memory_space=pltpu.HBM)] * 7,
        out_specs=(vmem, vmem, vmem),
        scratch_shapes=[
            pltpu.VMEM((B, I), I32),
            pltpu.VMEM((B, I), F32),
            pltpu.VMEM((K, I), I32),
            pltpu.VMEM(descriptors.shape, BF16),
            pltpu.SMEM(keypoint_count.shape, I32),
            pltpu.SMEM((W, C, S), I32),
            pltpu.SMEM((W, C, S), I32),
            pltpu.SMEM((2, pairs), I32),
            pltpu.VMEM((W * S, C, feats, width), BF16),
            pltpu.VMEM((W, S, C, feats, width), BF16),
            pltpu.VMEM((TR + 2 * KP, I), BF16),
            pltpu.VMEM((KP, I), I32),
            pltpu.VMEM((W, 2 * B + 8, LANES), F32),
            pltpu.VMEM((W, ceil_to(J, 8), LANES), I32),
            pltpu.VMEM((TR, J * LANES), F32),
            pltpu.VMEM((TR, J * LANES), F32),
            pltpu.VMEM((W, NP, LANES), F32),
            pltpu.VMEM((W, NP, LANES), F32),
            pltpu.VMEM((W, width, C * width) if gram else (H, width, width), BF16),
            pltpu.VMEM((H, width, width), BF16),
            pltpu.VMEM((H, width, width), F32),
            pltpu.VMEM((H, 8, width), F32),
            pltpu.VMEM((H * H if gram else 1, 8, width), F32),
            pltpu.VMEM((H * H if gram else 1, 8, width), F32),
            pltpu.VMEM((pairs * 8, width), F32),
            pltpu.VMEM((pairs * 8, width), F32),
            pltpu.VMEM((pairs * 8, width), F32),
            pltpu.SemaphoreType.DMA,
            pltpu.SemaphoreType.DMA((W,)),
            pltpu.SemaphoreType.DMA,
            pltpu.SemaphoreType.DMA,
            pltpu.SemaphoreType.REGULAR((W,)),
        ],
        compiler_params=pltpu.CompilerParams(
            collective_id=0, has_side_effects=True, vmem_limit_bytes=LIMIT,
        ),
    )(*(pltpu.with_memory_space_constraint(operand, pltpu.HBM) for operand in (
        word_ids[0], word_weights[0], neighbours, descriptors,
        keypoint_count, jnp.swapaxes(send_table, 2, 3), jnp.swapaxes(pair_slots, 2, 3)[0, 0],
    )))
    similarity, nearest, margin = pl.pallas_call(
        finish,
        out_shape=tuple(jax.ShapeDtypeStruct(shape, F32) for shape in results),
        in_specs=[pl.BlockSpec(memory_space=pl.ANY)] * 3,
        out_specs=(pl.BlockSpec(memory_space=pltpu.HBM),) * 3,
        scratch_shapes=[pltpu.SemaphoreType.DMA],
        compiler_params=pltpu.CompilerParams(vmem_limit_bytes=LIMIT),
    )(*parts)
    return similarity, nearest[None, None], margin[None, None]


def solution(mesh):
    in_specs = (
        P("word", None, "groups"),
        P("word", None, "groups"),
        P(None, "groups"),
        P(("groups", "word"), "sub", None),
        P("groups"),
        P("groups", None, None, None),
        P(("groups", "word"), "sub", None, None),
    )
    out_specs = (
        P(("groups", "word", "sub"), None),
        P(("groups", "word"), "sub", None, None),
        P(("groups", "word"), "sub", None, None),
    )
    body = functools.partial(local, mesh.shape["word"], mesh.shape["sub"])
    return jax.shard_map(body, mesh=mesh, in_specs=in_specs, out_specs=out_specs, check_vma=False)
```

```python
import functools

import jax
import jax.numpy as jnp
from jax import lax
from jax.experimental import pallas as pl
from jax.experimental.pallas import tpu as pltpu
from jax.sharding import PartitionSpec as P

MESH = pl.DeviceIdType.MESH
LANES = 128
LIMIT = 40 * 1024 * 1024
F32, BF16, I32 = jnp.float32, jnp.bfloat16, jnp.int32


def ceil_to(value, step):
    return (value + step - 1) // step * step


def loop(count, limit, body):
    if count <= limit:
        for i in range(count):
            body(i)
    else:
        lax.fori_loop(0, count, lambda i, carry: (body(i), carry)[1], 0)


def pieces(x):
    first = x.astype(BF16)
    return first, (x - first.astype(F32)).astype(BF16)


def dot(a, b):
    return lax.dot_general(a, b, (((1,), (0,)), ((), ())), preferred_element_type=F32)


def onehot(want, rows):
    numbers = lax.broadcasted_iota(I32, (rows, want.shape[-1]), 0)
    return jnp.where(numbers == want, F32(1.0), F32(0.0)).astype(BF16)


def kernel(
    W, S, dims,
    ids_hbm, wts_hbm, nb_hbm, desc_hbm, cnt_hbm, tab_hbm, slot_hbm,
    sim_ref, near_ref, marg_ref,
    ids_ref, wts_ref, nb_ref, desc_ref, cnt_ref, to_ref, from_ref, slot_ref,
    outd, held, table, nbf, own, wanted, got_0, got_1, part_out, part_in,
    qs, rt, sqb, info, low_t, next_t, low_s, next_s, info_s,
    dsend, drecv, psend, precv, go,
):
    B, I, K, R, KK, J, C, TR, KP, NP, H = dims
    gots = got_0, got_1
    gram = qs.shape[0] == W
    me_g, me_w, me_s = lax.axis_index("groups"), lax.axis_index("word"), lax.axis_index("sub")
    n = W * S
    stored, feats, width = desc_ref.shape

    def turn(step):
        if isinstance(step, int) and step == 0:
            return me_w
        inner = early
        place = jnp.where(inner, W - me_w, me_w + W - W // 2) % W
        k = step - 1 + jnp.where(step > place, 1, 0)
        w = jnp.where(inner, W - k, W // 2 + k) % W
        return w if isinstance(step, int) else jnp.where(step == 0, me_w, w)

    def word_at(k):
        return k + jnp.where(me_w <= k, 1, 0)

    def sub_at(j):
        if S % 2:
            return (me_s + j) % S
        own_side = me_s // (S // 2) * (S // 2)
        if isinstance(j, int):
            return S // 2 - own_side + j if j < S // 2 else own_side + j - S // 2
        return jnp.where(j < S // 2, S // 2 - own_side + j, own_side + j - S // 2)

    def load(sem, source, target):
        return pltpu.make_async_copy(source, target, sem)

    first = [
        load(dsend, tab_hbm.at[me_w], to_ref),
        load(dsend, desc_hbm, desc_ref),
    ]
    rest = [
        load(psend, ids_hbm, ids_ref),
        load(psend, wts_hbm, wts_ref),
        load(psend, nb_hbm, nb_ref),
        load(psend, tab_hbm.at[:, me_w], from_ref),
        load(psend, cnt_hbm, cnt_ref),
        load(psend, slot_hbm, slot_ref),
    ]
    for copy in first:
        copy.start()

    def words(above, body):
        for_each = lambda k: pl.when((k >= me_w) if above else (k < me_w))(lambda: body(word_at(k)))
        loop(W - 1, 4, for_each)

    def subs(above, body):
        loop(S, 8, lambda s: pl.when((s > me_s) if above else (s < me_s))(lambda: body(s)))

    barrier = pltpu.get_barrier_semaphore()

    def signal(sem, w, s):
        pl.semaphore_signal(sem, inc=1, device_id=(me_g, w, s), device_id_type=MESH)

    half, mid = S // 2, W // 2
    paired = W > 1 and S > 1 and not W & (W - 1) and not S & (S - 1)
    below, above = jnp.logical_and(paired, me_w == mid - 1), jnp.logical_and(paired, me_w == mid)
    side = me_s // max(half, 1) * half

    subs(True, lambda s: signal(barrier, me_w, s))
    if paired:
        pl.when(above)(lambda: loop(half, 8, lambda j: signal(barrier, mid - 1, side + j)))
    words(True, lambda w: loop(S, 8, lambda s: signal(barrier, w, s)))
    for copy in rest:
        copy.start()
    lower = me_w * S + me_s + jnp.where(below, half, 0)
    pl.when(lower > 0)(lambda: pl.semaphore_wait(barrier, lower))
    def answer(w):
        mate = jnp.logical_and(above, w == mid - 1)
        if paired:
            pl.when(mate)(lambda: loop(half, 8, lambda j: signal(go.at[me_w], w, half - side + j)))
        pl.when(jnp.logical_not(mate))(lambda: loop(S, 8, lambda s: signal(go.at[me_w], w, s)))

    words(False, answer)
    subs(False, lambda s: signal(go.at[me_w], me_w, s))
    for copy in first:
        copy.wait()

    def pick(slot, w, s):
        for c in range(C):
            outd[slot, c] = desc_ref[to_ref[w, c, s]]

    loop(W - 1, 4, lambda k: loop(S, 8, lambda j: pick(k * S + j, word_at(k), sub_at(j))))
    loop(S, 8, lambda j: pick((W - 1) * S + j, me_w, sub_at(j)))
    for c in range(C):
        held[me_w, me_s, c] = desc_ref[to_ref[me_w, c, me_s]]

    def send(slot, w, s):
        pltpu.make_async_remote_copy(
            src_ref=outd.at[slot], dst_ref=held.at[me_w, me_s],
            send_sem=dsend, recv_sem=drecv.at[me_w],
            device_id=(me_g, w, s), device_id_type=MESH,
        ).start()

    def send_word(k, first=0, last=S):
        loop(last - first, 8, lambda j: send(k * S + first + j, word_at(k), sub_at(first + j)))

    def send_near(above):
        def each(j):
            s = sub_at(j)
            pl.when((s > me_s) if above else (s < me_s))(lambda: send((W - 1) * S + j, me_w, s))

        loop(S, 8, each)

    early = 2 * me_w < W - 1
    late = jnp.logical_not(early)
    left = me_s < half
    pl.when(jnp.logical_and(me_w > 0, left))(lambda: send_word(0, half, S))
    pl.when(me_w > 0)(lambda: send_word(0, 0, half))
    pl.when(jnp.logical_and(me_w > 0, jnp.logical_not(left)))(lambda: send_word(0, half, S))
    if paired:
        pl.when(below)(lambda: send_word(mid - 1, half, S))
    send_near(False)

    for copy in rest:
        copy.wait()

    ids = ids_ref[...]
    table[0:B] = (ids >> 8).astype(F32).astype(BF16)
    table[B : 2 * B] = (ids & 255).astype(F32).astype(BF16)
    for i, piece in enumerate(pieces(wts_ref[...])):
        table[(2 + i) * B : (3 + i) * B] = piece
    nbf[...] = jnp.zeros_like(nbf)
    nbf[0:K] = nb_ref[...]
    near_ids = nbf[...]
    table[TR : TR + KP] = (near_ids >> 8).astype(F32).astype(BF16)
    table[TR + KP : TR + 2 * KP] = (near_ids & 255).astype(F32).astype(BF16)

    chunk = min(I, 256)

    def self_norm(i):
        at = pl.ds(i * chunk if isinstance(i, int) else pl.multiple_of(i * chunk, chunk), chunk)
        here = ids_ref[:, at]
        total = jnp.zeros((B, chunk), F32)
        for a in range(B):
            total += jnp.where(here == ids_ref[a : a + 1, at], wts_ref[a : a + 1, at], F32(0.0))
        norm = jnp.sum(total * wts_ref[:, at], axis=0, keepdims=True)
        row = lax.broadcasted_iota(I32, (16, chunk), 0)
        block = jnp.zeros((16, chunk), F32)
        for k, piece in enumerate(pieces(norm)):
            block = jnp.where(row == k, piece.astype(F32), block)
        table[4 * B : TR, at] = block.astype(BF16)

    loop(I // chunk, 1, self_norm)

    def part_copy(d):
        w = word_at(d)
        return pltpu.make_async_remote_copy(
            src_ref=part_out.at[d], dst_ref=part_in.at[me_w - jnp.where(me_w > w, 1, 0)],
            send_sem=psend, recv_sem=precv,
            device_id=(me_g, w, me_s), device_id_type=MESH,
        )

    lane = lax.broadcasted_iota(I32, (1, LANES), 1)
    digit = lax.broadcasted_iota(I32, (KK, LANES), 0) == lax.broadcasted_iota(I32, (KK, LANES), 1) // R

    def order(i):
        d = (i + jnp.where(early, me_w, 0)) % max(W - 1, 1)
        if isinstance(i, int):
            return d if i < W - 1 else W - 1
        return jnp.where(i < W - 1, d, W - 1)

    def owned(i):
        d = order(i)
        w = jnp.where(d == W - 1, me_w, word_at(d))
        mine = dot(table[...], onehot((w * S + me_s) * R + lane % R, I))
        own[i, 0:B] = mine[0:B] * 256.0 + mine[B : 2 * B]
        own[i, B : 2 * B] = mine[2 * B : 3 * B] + mine[3 * B : 4 * B]
        own[i, 2 * B : 2 * B + 1] = mine[4 * B : 4 * B + 1] + mine[4 * B + 1 : 4 * B + 2]
        listed = mine[TR : TR + KP] * 256.0 + mine[TR + KP : TR + 2 * KP]
        for j in range(J):
            chosen = jnp.where(digit, listed[j * KK : (j + 1) * KK], F32(0.0))
            wanted[i, j : j + 1] = jnp.sum(chosen, axis=0, keepdims=True).astype(I32)

    def gather(i):
        got = gots[i % 2] if isinstance(i, int) else gots[0]
        for j in range(J):
            got[:, j * LANES : (j + 1) * LANES] = dot(table[0:TR], onehot(wanted[i, j : j + 1], I))

    def target(i):
        d = order(i)
        got = gots[i % 2] if isinstance(i, int) else gots[0]
        cols = [slice(j * LANES, (j + 1) * LANES) for j in range(J)]
        words_of = [got[0:B, c] * 256.0 + got[B : 2 * B, c] for c in cols]
        total = [jnp.zeros((B, LANES), F32) for c in cols]
        for a in range(B):
            word, weight = own[i, a : a + 1], own[i, B + a : B + a + 1]
            for j in range(J):
                total[j] += jnp.where(words_of[j] == word, weight, F32(0.0))
        for j, c in enumerate(cols):
            values = got[2 * B : 3 * B, c] + got[3 * B : 4 * B, c]
            part_out[d, j : j + 1] = jnp.sum(total[j] * values, axis=0, keepdims=True)
            norms = got[4 * B : 4 * B + 1, c] + got[4 * B + 1 : 4 * B + 2, c]
            part_out[d, J + j : J + j + 1] = norms
        part_out[d, 2 * J : 2 * J + 1] = own[i, 2 * B : 2 * B + 1]

    def far_sends():
        def each(k):
            @pl.when(k >= me_w)
            def _():
                pl.semaphore_wait(go.at[k + 1], S)
                send_word(k)

        loop(W - 1, 4, each)

    def after(i):
        d = order(i)
        if isinstance(i, int) and i == 0:
            pl.when(me_s < S - 1)(lambda: pl.semaphore_wait(go.at[me_w], S - 1 - me_s))
            send_near(True)
            pl.when(late)(far_sends)
        high = me_w + 1 + i < W
        wait_high = jnp.logical_and(early, high)
        mate = jnp.logical_and(below, i == 0)
        pl.when(wait_high)(lambda: pl.semaphore_wait(go.at[me_w + 1 + i], jnp.where(mate, half, S)))
        part_copy(d).start()
        full = jnp.logical_and(wait_high, jnp.logical_not(mate))
        pl.when(jnp.logical_and(full, left))(lambda: send_word(d, half, S))
        pl.when(wait_high)(lambda: send_word(d, 0, half))
        pl.when(jnp.logical_and(full, jnp.logical_not(left)))(lambda: send_word(d, half, S))
        rest_low = jnp.logical_and(jnp.logical_and(early, jnp.logical_not(high)), d > 0)
        pl.when(rest_low)(lambda: send_word(d))
        if isinstance(i, int) and i == 0:
            pl.when(jnp.logical_and(late, me_w > 2))(lambda: send_word(me_w - 1))
        else:
            held_back = jnp.logical_or(i < me_w - 1, jnp.logical_and(i == 1, me_w == 2))
            pl.when(jnp.logical_and(late, held_back))(lambda: send_word(i))

    loop(W, 4, owned)
    if W <= 4:
        gather(0)
        for i in range(W):
            target(i)
            if i + 1 < W:
                gather(i + 1)
                after(i)
    else:
        def step(i):
            gather(i)
            target(i)

        step(0)
        after(0)
        lax.fori_loop(1, W - 1, lambda i, carry: (step(i), after(i), carry)[2], 0)
        step(W - 1)

    pairs = near_ref.shape[0]
    group = 8

    order_of = [turn(i) for i in range(W)] if gram else None

    def lowest_two(base, inner):
        tops = []
        for t in range(2):
            low = second = None
            for v in range(t, width // 8, 2):
                x = base[v * 8 : v * 8 + 8] + inner[v * 8 : v * 8 + 8]
                if low is None:
                    low = x
                elif second is None:
                    low, second = jnp.minimum(low, x), jnp.maximum(low, x)
                else:
                    second = jnp.minimum(second, jnp.maximum(low, x))
                    low = jnp.minimum(low, x)
            tops.append((low, second))
        (l0, s0), (l1, s1) = tops
        return jnp.minimum(l0, l1), jnp.minimum(jnp.maximum(l0, l1), jnp.minimum(s0, s1))

    def block(j, b):
        inner = dot(rt[b], qs[j])
        base = sqb[b]
        for c in range(C):
            a = j * C + c
            if a != b:
                cell = (order_of[j] * C + c) * H + order_of[b // C] * C + b % C
                low_t[cell], next_t[cell] = lowest_two(base, inner[:, c * width : (c + 1) * width])

    def arrive(i):
        w = order_of[i] if gram else turn(i)

        def arrived(slices):
            pltpu.make_async_remote_copy(
                src_ref=held.at[w, pl.ds(0, slices)], dst_ref=held.at[w, pl.ds(0, slices)],
                send_sem=dsend, recv_sem=drecv.at[w],
                device_id=(me_g, me_w, me_s), device_id_type=MESH,
            ).wait_recv()

        if isinstance(i, int):
            arrived(S if i > 0 else S - 1)
        else:
            pl.when(i > 0)(lambda: arrived(S))
            pl.when(i == 0)(lambda: arrived(S - 1))
        for c in range(C):
            h = i * C + c if gram else w * C + c
            full = jnp.concatenate([held[w, s, c] for s in range(S)], axis=0)
            if gram:
                qs[i, :, c * width : (c + 1) * width] = full
            else:
                qs[h] = full
            wide = full.astype(F32)
            turned = jnp.transpose(wide)
            rt[h] = (turned * -2.0).astype(BF16)
            count = cnt_ref[w * stored + from_ref[w, c, me_s]]
            down = lax.broadcasted_iota(I32, (width, width), 0)
            square = jnp.sum(turned * turned, axis=1, keepdims=True)
            sqb[h] = jnp.where(down < count, square, F32(1e30))
            flat = jnp.sum(wide * wide, axis=0, keepdims=True)
            live = jnp.where(lax.broadcasted_iota(I32, (8, width), 1) < count, F32(1.0), F32(0.0))
            info[w * C + c] = jnp.where(lax.broadcasted_iota(I32, (8, width), 0) == 0, flat, live)
        if gram:
            for b in range((i + 1) * C):
                block(i, b)
            for j in range(i):
                for c in range(C):
                    block(j, i * C + c)

    def whole(ref, send_sem, recv_sem):
        return pltpu.make_async_remote_copy(
            src_ref=ref, dst_ref=ref, send_sem=send_sem, recv_sem=recv_sem,
            device_id=(me_g, me_w, me_s), device_id_type=MESH,
        )

    def similarity():
        whole(part_in.at[pl.ds(0, W - 1)], psend, precv).wait_recv()
        total = part_out[W - 1]
        for d in range(W - 1):
            total += part_in[d]
        cosine = total[0:J] / jnp.sqrt(total[2 * J : 2 * J + 1] * total[J : 2 * J])
        spread = lax.broadcasted_iota(I32, (R, LANES), 1) % R == lax.broadcasted_iota(I32, (R, LANES), 0)
        out_cols = ceil_to(K, LANES)
        deep = lax.broadcasted_iota(I32, (LANES, out_cols), 0) // R
        across = lax.broadcasted_iota(I32, (LANES, out_cols), 1)
        result = jnp.zeros((R, out_cols), F32)
        for j in range(J):
            place = jnp.where(across == deep + j * KK, F32(1.0), F32(0.0)).astype(BF16)
            for piece in pieces(jnp.where(spread, cosine[j : j + 1], F32(0.0))):
                result += dot(piece, place)
        sim_ref[...] = result[:, 0:K]

    if 2 < W <= 4:
        arrive(0)
        arrive(1)
        pl.when(me_w % 2 == 1)(similarity)
        loop(W - 3, 4, lambda i: arrive(2 + i))
        pl.when(jnp.logical_and(me_w % 2 == 0, me_w > 0))(similarity)
        arrive(W - 1)
        pl.when(me_w == 0)(similarity)
    else:
        loop(W - 1, 4, arrive)
        similarity()
        arrive(W - 1)

    def match(i):
        for k in range(group):
            p = i * group + k
            a, b = slot_ref[0, p], slot_ref[1, p]
            at = pl.ds(p * 8, 8)
            if gram:
                low_s[at], next_s[at] = low_t[a * H + b], next_t[a * H + b]
            else:
                low_s[at], next_s[at] = lowest_two(sqb[b], dot(rt[b], qs[a]))
            info_s[at] = info[a]

    loop(pairs // group, 4, match)

    rows = [pl.ds(i, pairs, stride=8) for i in range(8)]
    low, second = low_s[rows[0]], next_s[rows[0]]
    for at in rows[1:]:
        l1, s1 = low_s[at], next_s[at]
        second = jnp.minimum(jnp.maximum(low, l1), jnp.minimum(second, s1))
        low = jnp.minimum(low, l1)
    live = info_s[rows[1]] > 0.0
    scale = F32(1.0 / (feats * S))
    near_ref[...] = jnp.where(live, (low + info_s[rows[0]]) * scale, F32(0.0))
    marg_ref[...] = jnp.where(live, (second - low) * scale, F32(0.0))

    whole(outd.at[pl.ds(0, n - 1)], dsend, drecv.at[0]).wait_send()
    whole(part_out.at[pl.ds(0, W - 1)], psend, precv).wait_send()


def finish(*refs):
    sems = refs[6]
    copies = [pltpu.make_async_copy(refs[i], refs[3 + i], sems.at[i]) for i in range(3)]
    for copy in copies:
        copy.start()
    for copy in copies:
        copy.wait()


def local(W, S, word_ids, word_weights, neighbours, descriptors, keypoint_count, send_table, pair_slots):
    B, I = word_ids.shape[1:]
    K = neighbours.shape[0]
    R = I // (W * S)
    KK = LANES // R
    J = -(-K // KK)
    C = send_table.shape[-1]
    TR = ceil_to(4 * B + 2, 16)
    KP = ceil_to(J * KK, 16)
    NP = ceil_to(2 * J + 1, 8)
    H = W * C
    stored, feats, width = descriptors.shape
    pairs = pair_slots.shape[2]
    gram = W <= 4 and C > 1 and H * H <= 2 * pairs
    vmem = pl.BlockSpec(memory_space=pltpu.VMEM)
    results = ((R, K), (pairs, width), (pairs, width))
    parts = pl.pallas_call(
        functools.partial(kernel, W, S, (B, I, K, R, KK, J, C, TR, KP, NP, H)),
        out_shape=tuple(pltpu.VMEM(shape, F32) for shape in results),
        in_specs=[pl.BlockSpec(memory_space=pltpu.HBM)] * 7,
        out_specs=(vmem, vmem, vmem),
        scratch_shapes=[
            pltpu.VMEM((B, I), I32),
            pltpu.VMEM((B, I), F32),
            pltpu.VMEM((K, I), I32),
            pltpu.VMEM(descriptors.shape, BF16),
            pltpu.SMEM(keypoint_count.shape, I32),
            pltpu.SMEM((W, C, S), I32),
            pltpu.SMEM((W, C, S), I32),
            pltpu.SMEM((2, pairs), I32),
            pltpu.VMEM((W * S, C, feats, width), BF16),
            pltpu.VMEM((W, S, C, feats, width), BF16),
            pltpu.VMEM((TR + 2 * KP, I), BF16),
            pltpu.VMEM((KP, I), I32),
            pltpu.VMEM((W, 2 * B + 8, LANES), F32),
            pltpu.VMEM((W, ceil_to(J, 8), LANES), I32),
            pltpu.VMEM((TR, J * LANES), F32),
            pltpu.VMEM((TR, J * LANES), F32),
            pltpu.VMEM((W, NP, LANES), F32),
            pltpu.VMEM((W, NP, LANES), F32),
            pltpu.VMEM((W, width, C * width) if gram else (H, width, width), BF16),
            pltpu.VMEM((H, width, width), BF16),
            pltpu.VMEM((H, width, width), F32),
            pltpu.VMEM((H, 8, width), F32),
            pltpu.VMEM((H * H if gram else 1, 8, width), F32),
            pltpu.VMEM((H * H if gram else 1, 8, width), F32),
            pltpu.VMEM((pairs * 8, width), F32),
            pltpu.VMEM((pairs * 8, width), F32),
            pltpu.VMEM((pairs * 8, width), F32),
            pltpu.SemaphoreType.DMA,
            pltpu.SemaphoreType.DMA((W,)),
            pltpu.SemaphoreType.DMA,
            pltpu.SemaphoreType.DMA,
            pltpu.SemaphoreType.REGULAR((W,)),
        ],
        compiler_params=pltpu.CompilerParams(
            collective_id=0, has_side_effects=True, vmem_limit_bytes=LIMIT
        ),
    )(*(pltpu.with_memory_space_constraint(operand, pltpu.HBM) for operand in (
        word_ids[0], word_weights[0], neighbours, descriptors,
        keypoint_count, jnp.swapaxes(send_table, 2, 3), jnp.swapaxes(pair_slots, 2, 3)[0, 0],
    )))
    similarity, nearest, margin = pl.pallas_call(
        finish,
        out_shape=tuple(jax.ShapeDtypeStruct(shape, F32) for shape in results),
        in_specs=[pl.BlockSpec(memory_space=pl.ANY)] * 3,
        out_specs=(pl.BlockSpec(memory_space=pltpu.HBM),) * 3,
        scratch_shapes=[pltpu.SemaphoreType.DMA((3,))],
        compiler_params=pltpu.CompilerParams(vmem_limit_bytes=LIMIT),
    )(*parts)
    return similarity, nearest[None, None], margin[None, None]


def solution(mesh):
    in_specs = (
        P("word", None, "groups"),
        P("word", None, "groups"),
        P(None, "groups"),
        P(("groups", "word"), "sub", None),
        P("groups"),
        P("groups", None, None, None),
        P(("groups", "word"), "sub", None, None),
    )
    out_specs = (
        P(("groups", "word", "sub"), None),
        P(("groups", "word"), "sub", None, None),
        P(("groups", "word"), "sub", None, None),
    )
    body = functools.partial(local, mesh.shape["word"], mesh.shape["sub"])
    return jax.shard_map(body, mesh=mesh, in_specs=in_specs, out_specs=out_specs, check_vma=False)
```
